256 devices in a mesh: shuf: 64 (over y, z, core), rep: 4 (over x).
Axes of the slice: x: 4, y: 4, z: 8, core: 2. Of those that a mesh axis runs over, the one named last changes fastest.
Arguments:
- values: bfloat16 [524288, 1024], P('shuf', 'rep')
- subgroup: int32 [4096], P('shuf'), may hold values from 0 to 31
- owners: int32 [4096, 1], P('shuf'), may hold values from 0 to 63; in each aligned block of 64 rows (0 to 63, 64 to 127, ...) at most 2 rows name the same one
- col_gain: float32 [1024], P('rep'), may hold values from 0.5 to 1.5
- col_bias: float32 [1024], P('rep'), may hold values from -3 to 3
- out_weight: bfloat16 [1024, 1024], P('rep'), may hold values from -0.1875 to 0.1875
Outputs:
- projected: bfloat16 [524288, 1024], P(('shuf', 'rep'))
The draws below stay inside these ranges and needn't reach their ends.
Inputs may be any that keep to these rules, and one draw needn't show every extreme that they name: `owners`: among the tiles of one index of shuf no owner is named more than 2 times, a bound that some block reaches.
All inputs are finite; a program needn't handle non-finite values.
Results may differ from the reference program's by a relative error of at most 0.015.
Values may be sent and summed in bfloat16 or wider, within the bound.
A program may use at most 64 MiB of HBM per device.

```python
import math
import jax
import jax.numpy as jnp
import numpy as np
from jax import lax

TILE = 128
TILES_DEV = 64
COLS = 1024
OUT = 1024
GRP_DEV = 32
PRIOR = 256
ROWS_DEV = 8192
TILES = 4096
ROWS = 524288
CAP = 2
N_SHUF = 64
N_REP = 4


def draw_values(key, part):
    keys = jax.random.split(jax.random.fold_in(key, 11), 7)
    blocks = ROWS // ROWS_DEV
    place = jnp.arange(ROWS, dtype=jnp.float32).reshape(TILES, TILE, 1) / float(ROWS)
    rough = jax.random.uniform(keys[0], (TILES, TILE, 1), minval=0.7, maxval=1.4)
    row_scale = jnp.exp(jnp.log(3.0) * place) * rough
    shift = 1.5 * jax.random.normal(keys[4], (blocks, 1, COLS))
    shift_rows = jnp.repeat(shift, TILES_DEV, axis=0)
    chosen = jax.random.bernoulli(keys[5], 0.5, (TILES, 1, COLS))
    stretch = jnp.exp(jax.random.uniform(keys[6], (TILES, 1, COLS), minval=-0.6, maxval=0.6))
    factor = jnp.where(chosen, stretch, 1.0)
    col_scale = jnp.exp(jax.random.uniform(keys[1], (1, 1, COLS), minval=0.0, maxval=jnp.log(10.0)))
    noise = jax.random.normal(keys[2], (TILES, TILE, COLS))
    offset = jax.random.normal(keys[3], (1, 1, COLS)) * (0.5 + 2.0 * place)
    drawn = col_scale * (offset + shift_rows + row_scale * noise * factor)
    return drawn.reshape(ROWS, COLS).astype(jnp.bfloat16)


def set_ends(values, stream_key, low, largest):
    spot = [jax.random.randint(jax.random.fold_in(stream_key, axis), (), 0, length) for axis, length in enumerate(values.shape)]
    widest = values.shape.index(max(values.shape))
    beside = spot[:widest] + [(spot[widest] + 1) % values.shape[widest]] + spot[widest + 1:]
    return values.at[tuple(spot)].set(low).at[tuple(beside)].set(largest)


def level_of(own_key, dims, pieces, smallest, high):
    gain, own = 1.0, jax.random.fold_in(own_key, 6)
    for axis_at, parts in pieces:
        heights = jnp.exp(jax.random.uniform(jax.random.fold_in(own, axis_at), (parts,), jnp.float32, smallest / len(pieces), high / len(pieces)))
        gain = gain * jnp.repeat(heights, dims[axis_at] // parts).reshape([-1 if axis == axis_at else 1 for axis in range(len(dims))])
    return gain


def assign_block(key, own, number, rows, amount, top, most, slope):
    sequence = jax.random.permutation(key, amount)
    heavy_load, ordinary = load_shares(amount, rows * top, most, slope, True), load_shares(amount, rows * top, most, slope, False)
    places = jnp.arange(amount)

    def named(tallies, offset_by):
        used = int((tallies > 0).sum())
        fixed = max(1, used // 4)
        passed = fixed + (places - fixed + offset_by * (used - fixed)) % max(1, amount - fixed)
        return jnp.zeros((amount,), jnp.int32).at[sequence[jnp.where(places < fixed, places, passed)]].set(jnp.asarray(tallies, jnp.int32))

    tallies = jnp.where(number % 4 == 0, named(heavy_load, number // 4), named(ordinary, number - number // 4 - 1))
    mixed = jax.random.permutation(jax.random.fold_in(own, 3), amount)
    source_of, sink = mixed[0:amount // 2 * 2:2], mixed[1:amount // 2 * 2:2]
    margin = jnp.minimum(tallies[source_of] - 1, most - tallies[sink]) // 2
    margin = jnp.where((source_of == sequence[0]) | (sink == sequence[0]) | (tallies[sink] == 0), 0, jnp.maximum(margin, 0))
    passed = jax.random.randint(jax.random.fold_in(own, 4), (amount // 2,), 0, 1 << 20) % (margin + 1)
    tallies = tallies.at[source_of].add(-passed).at[sink].add(passed)
    labels = jnp.searchsorted(jnp.cumsum(tallies), jnp.arange(rows * top), side="right").astype(jnp.int32)
    listing = labels.reshape(top, rows).T
    listing = listing[jax.random.permutation(jax.random.fold_in(own, 1), rows)]
    offset_by = jax.random.randint(jax.random.fold_in(own, 2), (rows, 1), 0, top)
    return jnp.take_along_axis(listing, (jnp.arange(top)[None, :] + offset_by) % top, axis=1)


def load_shares(count, total, limit, slope, full):
    portions = [(1 << 20) // math.isqrt(rank ** slope) + 1 for rank in range(1, count + 1)]
    largest = limit if full else min(limit, max(-(-total // count), total * portions[0] // sum(portions)))
    least = 1 if total - largest >= count - 1 else 0
    counts, surplus = [largest] + [least] * (count - 1), total - largest - least * (count - 1)
    while surplus > 0:
        movable = [i for i in range(1, count) if counts[i] < largest] or [i for i in range(1, count) if counts[i] < limit]
        whole, remaining = sum([portions[i] for i in movable]), surplus
        for i in movable:
            more = min(limit - counts[i], max(1, remaining * portions[i] // whole), surplus)
            counts[i] = counts[i] + more
            surplus = surplus - more
    return np.array(counts)


def normal_values(stream_key, extent, scale, reach, shards=(), held_as=jnp.bfloat16):
    result = scale * jax.random.normal(stream_key, extent, jnp.float32)
    if shards:
        result = result * level_of(stream_key, extent, shards, -0.22, 0.18)
    return jnp.clip(result, -reach, reach).astype(held_as)


def setup_inputs(seed: int = 0) -> dict:
    key_list = jax.random.split(jax.random.key(seed), 7)
    values = draw_values(jax.random.fold_in(key_list[6], 71), 0)
    subgroup = set_ends(jax.random.randint(key_list[1], (TILES,), 0, GRP_DEV), jax.random.fold_in(key_list[1], 1), 0, GRP_DEV - 1).astype(jnp.int32)
    owners_keys = jax.random.split(jax.random.fold_in(key_list[2], 1), TILES // TILES_DEV)
    owners_turns = jax.random.permutation(jax.random.fold_in(key_list[2], 3), TILES // TILES_DEV)
    owners = jax.vmap(lambda own, number: assign_block(jax.random.fold_in(key_list[2], 2), own, number, TILES_DEV, N_SHUF, 1, CAP, 1))(owners_keys, owners_turns).reshape((TILES, 1))
    col_gain = jnp.clip(1.0 + 0.1 * jax.random.normal(key_list[3], (COLS,), jnp.float32), 0.5, 1.5)
    col_bias = normal_values(key_list[4], (COLS,), 0.5, 3.0, ((0, 4),), jnp.float32)
    out_weight = normal_values(key_list[5], (COLS, OUT), COLS ** -0.5, 0.1875, ((0, 4),))
    return {"values": values, "subgroup": subgroup, "owners": owners, "col_gain": col_gain, "col_bias": col_bias, "out_weight": out_weight}


def reference(values, subgroup, owners, col_gain, col_bias, out_weight):
    row_total, col_total = values.shape
    tile_total = row_total // TILE
    groups = GRP_DEV * N_SHUF
    group = (owners[:, 0] * GRP_DEV + subgroup).astype(jnp.int32)
    shaped = values.astype(jnp.float32).reshape(tile_total, TILE, col_total)
    tile_sum = lax.optimization_barrier(jnp.sum(shaped, axis=1))
    tile_sq = lax.optimization_barrier(jnp.sum(shaped * shaped, axis=1))
    group_sum = jax.ops.segment_sum(tile_sum, group, num_segments=groups)
    group_sq = jax.ops.segment_sum(tile_sq, group, num_segments=groups)
    count = jax.ops.segment_sum(jnp.full((tile_total,), float(TILE), jnp.float32), group, num_segments=groups)
    mean_all = lax.optimization_barrier(jnp.sum(tile_sum, axis=0)) / float(row_total)
    square_all = lax.optimization_barrier(jnp.sum(tile_sq, axis=0)) / float(row_total)
    weight = (count + float(PRIOR))[:, None]
    center = (group_sum + float(PRIOR) * mean_all) / weight
    second = (group_sq + float(PRIOR) * square_all) / weight
    inverse = lax.rsqrt(second - center * center + 1e-05)
    tile_center = center[group]
    tile_scale = inverse[group] * col_gain
    scored = ((shaped - tile_center[:, None, :]) * tile_scale[:, None, :] + col_bias).astype(jnp.bfloat16)
    scored = scored.reshape(row_total, col_total)
    block_cols = col_total // N_REP
    summed = jnp.zeros((row_total, out_weight.shape[1]), jnp.float32)
    for block in range(N_REP):
        partial_value = jnp.dot(scored[:, block * block_cols:(block + 1) * block_cols], out_weight[block * block_cols:(block + 1) * block_cols], preferred_element_type=jnp.float32)
        summed = summed + partial_value.astype(jnp.bfloat16).astype(jnp.float32)
    return summed.astype(jnp.bfloat16)
```

```python
import jax
import jax.numpy as jnp
from jax import lax
from jax.experimental import pallas as pl
from jax.experimental.pallas import tpu as pltpu
from jax.sharding import PartitionSpec as P

TILE = 128
TILES = 64
GRP_DEV = 32
PRIOR = 256.0
COLS = 256
OUT = 1024
ROWS = 8192
OROWS = 2048
NX, NY, NZ, NC = 4, 4, 8, 2
NQ = NY * NC
SLOTS = 2 * NQ * NZ
GRPS = 8
GROWS = OROWS // GRPS
EARLY = 6
MSG = 2 * COLS + 128
MESH = pl.DeviceIdType.MESH
F32, BF16 = jnp.float32, jnp.bfloat16


def shuf_index(y, z, c):
    return (y * NZ + z) * NC + c


def iota(shape, dim):
    return lax.broadcasted_iota(jnp.int32, shape, dim)


def pick(matrix, rows):
    return jnp.dot(matrix, rows, preferred_element_type=F32)


def exchange(
    values, subgroup, owners, gain, bias, weight,
    out,
    vals, raw, wall, subs, owns, gb, tstat, totals, tot_y, tot_z,
    send_y, buf_y, send_z, buf_z, back_z, got_z, back_y, got_y, tile_stat, peer_stat, par, lhs,
    load_sem, aux_sem, x_send, x_recv, wx_send, wx_recv, wz_send, wz_recv, wy_send, wy_recv,
    wc_send, wc_recv, gb_send, gb_recv, st_send, st_recv, line_send, line_recv, near, far,
):
    shuf, x = lax.axis_index("shuf"), lax.axis_index("rep")
    y, z, c = shuf // (NZ * NC), lax.rem(shuf // NC, NZ), lax.rem(shuf, NC)
    q = y * NC + c
    barrier = pltpu.get_barrier_semaphore()

    def x_peer(d):
        return (shuf, lax.rem(x + d, NX))

    def z_peer(d):
        return (shuf_index(y, lax.rem(z + d, NZ), c), x)

    def q_peer(d):
        p = lax.rem(q + d, NQ)
        return (shuf_index(p // NC, z, lax.rem(p, NC)), x)

    def signal(sem, to):
        pl.semaphore_signal(sem, inc=1, device_id=to, device_id_type=MESH)

    def send(src, dst, s, r, to):
        pltpu.make_async_remote_copy(src, dst, s, r, device_id=to, device_id_type=MESH).start()

    def wait_for(ref, sem):
        pltpu.make_async_copy(ref, ref, sem).wait()

    @pl.when(x == 0)
    def _():
        for d in range(1, NX):
            signal(barrier, x_peer(d))

    @pl.when(x != 0)
    def _():
        for d in range(1, NX):
            @pl.when(x + d != NX)
            def _():
                signal(barrier, x_peer(d))
        pl.semaphore_wait(barrier, NX - 1)
        signal(near, (shuf, 0))

    @pl.when(x == 0)
    def _():
        pl.semaphore_wait(near, NX - 1)

    w_rows = pl.ds(pl.multiple_of((c * NZ + z) * 16, 16), 16)
    w_cols = pl.ds(pl.multiple_of(y * 256, 256), 256)
    for d in range(1, NX):
        at = NX - d
        send(
            weight.at[w_rows, w_cols],
            wall.at[pl.ds(pl.multiple_of(at * COLS + (c * NZ + z) * 16, 16), 16), w_cols],
            wx_send, wx_recv, x_peer(d),
        )
        send(gain, gb.at[at, 0], gb_send, gb_recv, x_peer(d))
        send(bias, gb.at[at, 1], gb_send, gb_recv, x_peer(d))

    def send_group(g):
        for d in (2, 1, 3):
            first = lax.rem(x + d, NX) * OROWS + g * GROWS
            send(
                values.at[pl.ds(pl.multiple_of(first, GROWS), GROWS)],
                raw.at[NX - d - 1, pl.ds(g * GROWS, GROWS)],
                x_send, x_recv.at[NX - d - 1, g], x_peer(d),
            )

    for g in range(EARLY):
        send_group(g)

    @pl.when(x == 0)
    def _():
        for d in range(1, NQ):
            signal(barrier, q_peer(d))
        for d in range(1, NZ):
            signal(barrier, z_peer(d))

    loads = []
    for i in range(8):
        part = pl.ds(i * 1024, 1024)
        loads.append(pltpu.make_async_copy(values.at[part], vals.at[part], load_sem.at[i]))
        loads[-1].start()
    aux = [
        pltpu.make_async_copy(subgroup, subs, aux_sem.at[0]),
        pltpu.make_async_copy(owners, owns, aux_sem.at[1]),
        pltpu.make_async_copy(weight, wall.at[pl.ds(0, COLS)], aux_sem.at[2]),
        pltpu.make_async_copy(gain, gb.at[0, 0], aux_sem.at[3]),
        pltpu.make_async_copy(bias, gb.at[0, 1], aux_sem.at[4]),
    ]
    for a in aux:
        a.start()

    @pl.loop(0, 8)
    def _(i):
        wait_for(vals.at[pl.ds(0, 1024)], load_sem.at[i])

        @pl.loop(0, 8)
        def _(j):
            t = i * 8 + j
            a = jnp.zeros((8, COLS), F32)
            b = jnp.zeros((8, COLS), F32)
            for k in range(TILE // 16):
                v = vals[pl.ds(pl.multiple_of(t * TILE + k * 16, 16), 16), :].astype(F32)
                lo, hi = v[:8], v[8:]
                a = a + lo + hi
                b = b + lo * lo + hi * hi
            tstat[pl.ds(t, 1), :COLS] = jnp.sum(a, axis=0, keepdims=True)
            tstat[pl.ds(t, 1), COLS:] = jnp.sum(b, axis=0, keepdims=True)

    sums = tstat[...]
    own_total = jnp.sum(sums, axis=0, keepdims=True)
    totals[0] = own_total
    tot_y[q] = own_total

    for a in aux[:2]:
        a.wait()
    lane = iota((8, TILES), 1)
    own_row = jnp.zeros((8, TILES), jnp.int32)
    sub_row = jnp.zeros((8, TILES), jnp.int32)
    for t in range(TILES):
        own_row = jnp.where(lane == t, owns[t], own_row)
        sub_row = jnp.where(lane == t, subs[t], sub_row)
    i0, i1 = iota((TILES, TILES), 0), iota((TILES, TILES), 1)
    eye = i0 == i1

    def as_rows(row):
        return jnp.broadcast_to(row[:1], (TILES, TILES))

    def as_column(row):
        spread = jnp.where(eye, as_rows(row), 0).astype(F32)
        return jnp.sum(spread, axis=1, keepdims=True).astype(jnp.int32)

    same = (as_rows(own_row) == as_column(own_row)) & (i0 < i1)
    pos = jnp.sum(jnp.where(same, 1.0, 0.0), axis=0, keepdims=True).astype(jnp.int32)
    o = own_row[:1]
    slot = ((((o >> 4) * NC + (o & 1)) * NZ + ((o >> 1) & 7)) * 2) + pos
    slot_col = as_column(slot)
    to_slot = jnp.where(iota((SLOTS, TILES), 0) == slot, 1.0, 0.0).astype(BF16)
    from_slot = jnp.where(iota((TILES, SLOTS), 1) == slot_col, 1.0, 0.0).astype(BF16)
    label = jnp.where(iota((TILES, 128), 1) == as_column(sub_row), 1.0, 0.0).astype(BF16)
    packed = jnp.concatenate([sums.astype(BF16), label], axis=1)
    send_y[...] = pick(to_slot, packed).astype(BF16).reshape(NQ, 16, MSG)
    buf_y[q] = send_y[q]

    r0, r1 = iota((SLOTS, SLOTS), 0), iota((SLOTS, SLOTS), 1)
    swap = jnp.where(r1 == ((r0 >> 1) & 7) * 16 + (r0 >> 4) * 2 + (r0 & 1), 1.0, 0.0).astype(BF16)

    @pl.when(x == 0)
    def _():
        pl.semaphore_wait(barrier, NQ - 1 + NZ - 1)
        for d in range(1, NX):
            signal(far, x_peer(d))

    @pl.when(x != 0)
    def _():
        pl.semaphore_wait(far, 1)

    for d in range(1, NQ):
        p = lax.rem(q + d, NQ)
        send(totals.at[0], tot_y.at[q], line_send.at[0], line_recv.at[0], q_peer(d))
        send(send_y.at[p], buf_y.at[q], line_send.at[1], line_recv.at[1], q_peer(d))

    wait_for(wall.at[pl.ds(0, 48), pl.ds(0, 256)], wx_recv)
    for d in range(1, NZ):
        for b in range(1, NX):
            piece = wall.at[pl.ds(pl.multiple_of(b * COLS + (c * NZ + z) * 16, 16), 16), w_cols]
            send(piece, piece, wz_send, wz_recv, z_peer(d))

    wait_for(tot_y.at[pl.ds(0, NQ - 1)], line_recv.at[0])
    wait_for(buf_y.at[pl.ds(0, NQ - 1)], line_recv.at[1])
    line_total = jnp.sum(tot_y[...], axis=0)
    totals[1] = line_total
    tot_z[z] = line_total
    send_z[...] = pick(swap, buf_y[...].reshape(SLOTS, MSG)).astype(BF16).reshape(NZ, 16, MSG)
    buf_z[z] = send_z[z]
    for d in range(1, NZ):
        p = lax.rem(z + d, NZ)
        send(totals.at[1], tot_z.at[z], line_send.at[2], line_recv.at[2], z_peer(d))
        send(send_z.at[p], buf_z.at[z], line_send.at[3], line_recv.at[3], z_peer(d))

    wait_for(wall.at[pl.ds(0, (NX - 1) * (NZ - 1) * 16), pl.ds(0, 256)], wz_recv)
    for d in range(1, NY):
        for b in range(1, NX):
            piece = wall.at[pl.ds(pl.multiple_of(b * COLS + c * 128, 128), 128), w_cols]
            send(piece, piece, wy_send, wy_recv, q_peer(NC * d))

    wait_for(tot_z.at[pl.ds(0, NZ - 1)], line_recv.at[2])
    wait_for(buf_z.at[pl.ds(0, NZ - 1)], line_recv.at[3])
    total = jnp.sum(tot_z[...], axis=0) / float(ROWS * NQ * NZ)
    arrived = buf_z[...].reshape(SLOTS, MSG)
    member = arrived[:, 2 * COLS:]
    member_t = jnp.transpose(member.astype(F32))[:GRP_DEV].astype(BF16)
    group = pick(member_t, arrived[:, : 2 * COLS])
    count = float(TILE) * jnp.sum(member_t.astype(F32), axis=1, keepdims=True)
    blended = (group + PRIOR * total) / (count + PRIOR)
    center, second = blended[:, :COLS], blended[:, COLS:]
    inverse = lax.rsqrt(second - center * center + 1e-05)
    both = jnp.concatenate([center, inverse], axis=1).astype(BF16)
    both = jnp.concatenate([both, jnp.zeros((128 - GRP_DEV, 2 * COLS), BF16)], axis=0)
    back_z[...] = pick(member, both).astype(BF16).reshape(NZ, 16, 2 * COLS)
    got_z[z] = back_z[z]
    for d in range(1, NZ):
        p = lax.rem(z + d, NZ)
        send(back_z.at[p], got_z.at[z], line_send.at[4], line_recv.at[4], z_peer(d))

    wait_for(got_z.at[pl.ds(0, NZ - 1)], line_recv.at[4])
    back_y[...] = pick(swap, got_z[...].reshape(SLOTS, 2 * COLS)).astype(BF16).reshape(NQ, 16, 2 * COLS)
    got_y[q] = back_y[q]
    for d in range(1, NQ):
        p = lax.rem(q + d, NQ)
        send(back_y.at[p], got_y.at[q], line_send.at[5], line_recv.at[5], q_peer(d))

    wait_for(wall.at[pl.ds(0, 3 * 128), pl.ds(0, 768)], wy_recv)
    for b in range(1, NX):
        piece = wall.at[pl.ds(pl.multiple_of(b * COLS + c * 128, 128), 128)]
        send(piece, piece, wc_send, wc_recv, (shuf_index(y, z, 1 - c), x))

    wait_for(got_y.at[pl.ds(0, NQ - 1)], line_recv.at[5])
    tile_stat[...] = pick(from_slot, got_y[...].reshape(SLOTS, 2 * COLS)).astype(BF16)
    for d in range(1, NX):
        rows = pl.ds(pl.multiple_of(lax.rem(x + d, NX) * 16, 16), 16)
        send(tile_stat.at[rows], peer_stat.at[NX - d - 1], st_send, st_recv, x_peer(d))
    for g in range(EARLY, GRPS):
        send_group(g)

    for a in aux[2:]:
        a.wait()
    wait_for(gb.at[pl.ds(0, NX - 1)], gb_recv)
    wait_for(wall.at[pl.ds(0, 3 * 128)], wc_recv)
    own_rows = pl.ds(pl.multiple_of(x * 16, 16), 16)
    stats = [tile_stat[own_rows, :]]
    wait_for(peer_stat, st_recv)
    stats += [peer_stat[d] for d in range(NX - 1)]
    for d in range(NX):
        s = stats[d].astype(F32)
        par[0, :, d * COLS:(d + 1) * COLS] = s[:, :COLS]
        par[1, :, d * COLS:(d + 1) * COLS] = s[:, COLS:] * gb[d, 0:1, :]

    @pl.loop(0, GRPS)
    def _(g):
        for d in range(1, NX):
            wait_for(raw.at[d - 1, pl.ds(0, GROWS)], x_recv.at[d - 1, g])
        for j in range(GROWS // TILE):
            t = g * (GROWS // TILE) + j
            for d in range(NX):
                cols = slice(d * COLS, (d + 1) * COLS)
                if d == 0:
                    first = x * OROWS + t * TILE
                    v = vals[pl.ds(pl.multiple_of(first, TILE), TILE), :]
                else:
                    v = raw[d - 1, pl.ds(pl.multiple_of(t * TILE, TILE), TILE), :]
                scored = (v.astype(F32) - par[0, pl.ds(t, 1), cols]) * par[1, pl.ds(t, 1), cols]
                lhs[j * TILE:(j + 1) * TILE, cols] = (scored + gb[d, 1:2, :]).astype(BF16)
        rows = pl.ds(pl.multiple_of(g * GROWS, GROWS), GROWS)
        out[rows, :] = jnp.dot(lhs[...], wall[...], preferred_element_type=F32).astype(BF16)

    wait_for(raw, x_send)
    wait_for(wall.at[pl.ds(0, 48), pl.ds(0, 256)], wx_send)
    wait_for(wall.at[pl.ds(0, (NX - 1) * (NZ - 1) * 16), pl.ds(0, 256)], wz_send)
    wait_for(wall.at[pl.ds(0, 3 * 128), pl.ds(0, 768)], wy_send)
    wait_for(wall.at[pl.ds(0, 3 * 128)], wc_send)
    wait_for(gb.at[pl.ds(0, NX - 1)], gb_send)
    wait_for(peer_stat, st_send)
    wait_for(tot_y.at[pl.ds(0, NQ - 1)], line_send.at[0])
    wait_for(buf_y.at[pl.ds(0, NQ - 1)], line_send.at[1])
    wait_for(tot_z.at[pl.ds(0, NZ - 1)], line_send.at[2])
    wait_for(buf_z.at[pl.ds(0, NZ - 1)], line_send.at[3])
    wait_for(got_z.at[pl.ds(0, NZ - 1)], line_send.at[4])
    wait_for(got_y.at[pl.ds(0, NQ - 1)], line_send.at[5])


def write_out(src, dst, sem):
    copies = []
    for i in range(4):
        rows = pl.ds(i * (OROWS // 4), OROWS // 4)
        copies.append(pltpu.make_async_copy(src.at[rows], dst.at[rows], sem.at[i]))
        copies[-1].start()
    for copy in copies:
        copy.wait()


def on_device(values, subgroup, owners, col_gain, col_bias, out_weight):
    dma, vmem = pltpu.SemaphoreType.DMA, pltpu.VMEM
    hbm = pl.BlockSpec(memory_space=pltpu.HBM)
    rows = pl.pallas_call(
        exchange,
        out_shape=pltpu.VMEM((OROWS, OUT), BF16),
        in_specs=[hbm] * 6,
        out_specs=pl.BlockSpec(memory_space=pltpu.VMEM),
        scratch_shapes=[
            vmem((ROWS, COLS), BF16),
            vmem((NX - 1, OROWS, COLS), BF16),
            vmem((NX * COLS, OUT), BF16),
            pltpu.SMEM((TILES,), jnp.int32),
            pltpu.SMEM((TILES,), jnp.int32),
            vmem((NX, 2, COLS), F32),
            vmem((TILES, 2 * COLS), F32),
            vmem((2, 1, 2 * COLS), F32),
            vmem((NQ, 1, 2 * COLS), F32),
            vmem((NZ, 1, 2 * COLS), F32),
            vmem((NQ, 16, MSG), BF16),
            vmem((NQ, 16, MSG), BF16),
            vmem((NZ, 16, MSG), BF16),
            vmem((NZ, 16, MSG), BF16),
            vmem((NZ, 16, 2 * COLS), BF16),
            vmem((NZ, 16, 2 * COLS), BF16),
            vmem((NQ, 16, 2 * COLS), BF16),
            vmem((NQ, 16, 2 * COLS), BF16),
            vmem((TILES, 2 * COLS), BF16),
            vmem((NX - 1, 16, 2 * COLS), BF16),
            vmem((2, 16, NX * COLS), F32),
            vmem((GROWS, NX * COLS), BF16),
            dma((8,)), dma((5,)), dma, dma((NX - 1, GRPS)),
            dma, dma, dma, dma, dma, dma, dma, dma, dma, dma, dma, dma,
            dma((6,)), dma((6,)),
            pltpu.SemaphoreType.REGULAR, pltpu.SemaphoreType.REGULAR,
        ],
        compiler_params=pltpu.CompilerParams(
            collective_id=0, has_side_effects=True, vmem_limit_bytes=32 * 1024 * 1024
        ),
    )(values, subgroup, owners.reshape(TILES), col_gain, col_bias, out_weight)
    return pl.pallas_call(
        write_out,
        out_shape=jax.ShapeDtypeStruct((OROWS, OUT), BF16),
        in_specs=[pl.BlockSpec(memory_space=pltpu.VMEM)],
        out_specs=pl.BlockSpec(memory_space=pltpu.HBM),
        scratch_shapes=[dma((4,))],
        compiler_params=pltpu.CompilerParams(vmem_limit_bytes=1024 * 1024),
    )(rows)


def solution(mesh):
    return jax.shard_map(
        on_device,
        mesh=mesh,
        in_specs=(P("shuf", "rep"), P("shuf"), P("shuf", None), P("rep"), P("rep"), P("rep", None)),
        out_specs=P(("shuf", "rep"), None),
        check_vma=False,
    )
```

```python
import jax
import jax.numpy as jnp
from jax import lax
from jax.experimental import pallas as pl
from jax.experimental.pallas import tpu as pltpu
from jax.sharding import PartitionSpec as P

TILE = 128
TILES = 64
GRP_DEV = 32
PRIOR = 256.0
COLS = 256
OUT = 1024
ROWS = 8192
OROWS = 2048
NX, NY, NZ, NC = 4, 4, 8, 2
NQ = NY * NC
SLOTS = 2 * NQ * NZ
GRPS = 8
GROWS = OROWS // GRPS
EARLY = 6
MSG = 2 * COLS + 128
MESH = pl.DeviceIdType.MESH
F32, BF16 = jnp.float32, jnp.bfloat16


def shuf_index(y, z, c):
    return (y * NZ + z) * NC + c


def iota(shape, dim):
    return lax.broadcasted_iota(jnp.int32, shape, dim)


def pick(matrix, rows):
    return jnp.dot(matrix, rows, preferred_element_type=F32)


def exchange(
    values, subgroup, owners, gain, bias, weight,
    out,
    vals, raw, wall, subs, owns, gb, tstat, totals, tot_y, tot_z,
    send_y, buf_y, send_z, buf_z, back_z, got_z, back_y, got_y, tile_stat, peer_stat, par, lhs,
    load_sem, aux_sem, x_send, x_recv, wx_send, wx_recv, wz_send, wz_recv, wy_send, wy_recv,
    wc_send, wc_recv, gb_send, gb_recv, st_send, st_recv, line_send, line_recv, near, far,
):
    shuf, x = lax.axis_index("shuf"), lax.axis_index("rep")
    y, z, c = shuf // (NZ * NC), lax.rem(shuf // NC, NZ), lax.rem(shuf, NC)
    q = y * NC + c
    barrier = pltpu.get_barrier_semaphore()

    def x_peer(d):
        return (shuf, lax.rem(x + d, NX))

    def z_peer(d):
        return (shuf_index(y, lax.rem(z + d, NZ), c), x)

    def q_peer(d):
        p = lax.rem(q + d, NQ)
        return (shuf_index(p // NC, z, lax.rem(p, NC)), x)

    def signal(sem, to):
        pl.semaphore_signal(sem, inc=1, device_id=to, device_id_type=MESH)

    def send(src, dst, s, r, to):
        pltpu.make_async_remote_copy(src, dst, s, r, device_id=to, device_id_type=MESH).start()

    def wait_for(ref, sem):
        pltpu.make_async_copy(ref, ref, sem).wait()

    @pl.when(x == 0)
    def _():
        for d in range(1, NX):
            signal(barrier, x_peer(d))

    @pl.when(x != 0)
    def _():
        for d in range(1, NX):
            @pl.when(x + d != NX)
            def _():
                signal(barrier, x_peer(d))
        pl.semaphore_wait(barrier, NX - 1)
        signal(near, (shuf, 0))

    @pl.when(x == 0)
    def _():
        pl.semaphore_wait(near, NX - 1)

    w_rows = pl.ds(pl.multiple_of((c * NZ + z) * 16, 16), 16)
    w_cols = pl.ds(pl.multiple_of(y * 256, 256), 256)
    for d in range(1, NX):
        at = NX - d
        send(
            weight.at[w_rows, w_cols],
            wall.at[pl.ds(pl.multiple_of(at * COLS + (c * NZ + z) * 16, 16), 16), w_cols],
            wx_send, wx_recv, x_peer(d),
        )
        send(gain, gb.at[at, 0], gb_send, gb_recv, x_peer(d))
        send(bias, gb.at[at, 1], gb_send, gb_recv, x_peer(d))

    def send_group(g):
        for d in (2, 1, 3):
            first = lax.rem(x + d, NX) * OROWS + g * GROWS
            send(
                values.at[pl.ds(pl.multiple_of(first, GROWS), GROWS)],
                raw.at[NX - d - 1, pl.ds(g * GROWS, GROWS)],
                x_send, x_recv.at[NX - d - 1, g], x_peer(d),
            )

    for g in range(EARLY):
        send_group(g)

    @pl.when(x == 0)
    def _():
        for d in range(1, NQ):
            signal(barrier, q_peer(d))
        for d in range(1, NZ):
            signal(barrier, z_peer(d))

    loads = []
    for i in range(8):
        part = pl.ds(i * 1024, 1024)
        loads.append(pltpu.make_async_copy(values.at[part], vals.at[part], load_sem.at[i]))
        loads[-1].start()
    aux = [
        pltpu.make_async_copy(subgroup, subs, aux_sem.at[0]),
        pltpu.make_async_copy(owners, owns, aux_sem.at[1]),
        pltpu.make_async_copy(weight, wall.at[pl.ds(0, COLS)], aux_sem.at[2]),
        pltpu.make_async_copy(gain, gb.at[0, 0], aux_sem.at[3]),
        pltpu.make_async_copy(bias, gb.at[0, 1], aux_sem.at[4]),
    ]
    for a in aux:
        a.start()

    @pl.loop(0, 8)
    def _(i):
        wait_for(vals.at[pl.ds(0, 1024)], load_sem.at[i])

        @pl.loop(0, 8)
        def _(j):
            t = i * 8 + j
            a = jnp.zeros((8, COLS), F32)
            b = jnp.zeros((8, COLS), F32)
            for k in range(TILE // 16):
                v = vals[pl.ds(pl.multiple_of(t * TILE + k * 16, 16), 16), :].astype(F32)
                lo, hi = v[:8], v[8:]
                a = a + lo + hi
                b = b + lo * lo + hi * hi
            tstat[pl.ds(t, 1), :COLS] = jnp.sum(a, axis=0, keepdims=True)
            tstat[pl.ds(t, 1), COLS:] = jnp.sum(b, axis=0, keepdims=True)

    sums = tstat[...]
    own_total = jnp.sum(sums, axis=0, keepdims=True)
    totals[0] = own_total
    tot_y[q] = own_total

    for a in aux[:2]:
        a.wait()
    lane = iota((8, TILES), 1)
    own_row = jnp.zeros((8, TILES), jnp.int32)
    sub_row = jnp.zeros((8, TILES), jnp.int32)
    for t in range(TILES):
        own_row = jnp.where(lane == t, owns[t], own_row)
        sub_row = jnp.where(lane == t, subs[t], sub_row)
    i0, i1 = iota((TILES, TILES), 0), iota((TILES, TILES), 1)
    eye = i0 == i1

    def as_rows(row):
        return jnp.broadcast_to(row[:1], (TILES, TILES))

    def as_column(row):
        spread = jnp.where(eye, as_rows(row), 0).astype(F32)
        return jnp.sum(spread, axis=1, keepdims=True).astype(jnp.int32)

    same = (as_rows(own_row) == as_column(own_row)) & (i0 < i1)
    pos = jnp.sum(jnp.where(same, 1.0, 0.0), axis=0, keepdims=True).astype(jnp.int32)
    o = own_row[:1]
    slot = ((((o >> 4) * NC + (o & 1)) * NZ + ((o >> 1) & 7)) * 2) + pos
    slot_col = as_column(slot)
    to_slot = jnp.where(iota((SLOTS, TILES), 0) == slot, 1.0, 0.0).astype(BF16)
    from_slot = jnp.where(iota((TILES, SLOTS), 1) == slot_col, 1.0, 0.0).astype(BF16)
    label = jnp.where(iota((TILES, 128), 1) == as_column(sub_row), 1.0, 0.0).astype(BF16)
    packed = jnp.concatenate([sums.astype(BF16), label], axis=1)
    send_y[...] = pick(to_slot, packed).astype(BF16).reshape(NQ, 16, MSG)
    buf_y[q] = send_y[q]

    r0, r1 = iota((SLOTS, SLOTS), 0), iota((SLOTS, SLOTS), 1)
    swap = jnp.where(r1 == ((r0 >> 1) & 7) * 16 + (r0 >> 4) * 2 + (r0 & 1), 1.0, 0.0).astype(BF16)

    @pl.when(x == 0)
    def _():
        pl.semaphore_wait(barrier, NQ - 1 + NZ - 1)
        for d in range(1, NX):
            signal(far, x_peer(d))

    @pl.when(x != 0)
    def _():
        pl.semaphore_wait(far, 1)

    for d in range(1, NQ):
        p = lax.rem(q + d, NQ)
        send(totals.at[0], tot_y.at[q], line_send.at[0], line_recv.at[0], q_peer(d))
        send(send_y.at[p], buf_y.at[q], line_send.at[1], line_recv.at[1], q_peer(d))

    wait_for(wall.at[pl.ds(0, 48), pl.ds(0, 256)], wx_recv)
    for d in range(1, NZ):
        for b in range(1, NX):
            piece = wall.at[pl.ds(pl.multiple_of(b * COLS + (c * NZ + z) * 16, 16), 16), w_cols]
            send(piece, piece, wz_send, wz_recv, z_peer(d))

    wait_for(tot_y.at[pl.ds(0, NQ - 1)], line_recv.at[0])
    wait_for(buf_y.at[pl.ds(0, NQ - 1)], line_recv.at[1])
    line_total = jnp.sum(tot_y[...], axis=0)
    totals[1] = line_total
    tot_z[z] = line_total
    send_z[...] = pick(swap, buf_y[...].reshape(SLOTS, MSG)).astype(BF16).reshape(NZ, 16, MSG)
    buf_z[z] = send_z[z]
    for d in range(1, NZ):
        p = lax.rem(z + d, NZ)
        send(totals.at[1], tot_z.at[z], line_send.at[2], line_recv.at[2], z_peer(d))
        send(send_z.at[p], buf_z.at[z], line_send.at[3], line_recv.at[3], z_peer(d))

    wait_for(wall.at[pl.ds(0, (NX - 1) * (NZ - 1) * 16), pl.ds(0, 256)], wz_recv)
    for d in range(1, NY):
        for b in range(1, NX):
            piece = wall.at[pl.ds(pl.multiple_of(b * COLS + c * 128, 128), 128), w_cols]
            send(piece, piece, wy_send, wy_recv, q_peer(NC * d))

    wait_for(tot_z.at[pl.ds(0, NZ - 1)], line_recv.at[2])
    wait_for(buf_z.at[pl.ds(0, NZ - 1)], line_recv.at[3])
    total = jnp.sum(tot_z[...], axis=0) / float(ROWS * NQ * NZ)
    arrived = buf_z[...].reshape(SLOTS, MSG)
    member = arrived[:, 2 * COLS:]
    member_t = jnp.transpose(member.astype(F32))[:GRP_DEV].astype(BF16)
    group = pick(member_t, arrived[:, : 2 * COLS])
    count = float(TILE) * jnp.sum(member_t.astype(F32), axis=1, keepdims=True)
    blended = (group + PRIOR * total) / (count + PRIOR)
    center, second = blended[:, :COLS], blended[:, COLS:]
    inverse = lax.rsqrt(second - center * center + 1e-05)
    both = jnp.concatenate([center, inverse], axis=1).astype(BF16)
    both = jnp.concatenate([both, jnp.zeros((128 - GRP_DEV, 2 * COLS), BF16)], axis=0)
    back_z[...] = pick(member, both).astype(BF16).reshape(NZ, 16, 2 * COLS)
    got_z[z] = back_z[z]
    for d in range(1, NZ):
        p = lax.rem(z + d, NZ)
        send(back_z.at[p], got_z.at[z], line_send.at[4], line_recv.at[4], z_peer(d))

    wait_for(got_z.at[pl.ds(0, NZ - 1)], line_recv.at[4])
    back_y[...] = pick(swap, got_z[...].reshape(SLOTS, 2 * COLS)).astype(BF16).reshape(NQ, 16, 2 * COLS)
    got_y[q] = back_y[q]
    for d in range(1, NQ):
        p = lax.rem(q + d, NQ)
        send(back_y.at[p], got_y.at[q], line_send.at[5], line_recv.at[5], q_peer(d))

    wait_for(wall.at[pl.ds(0, 3 * 128), pl.ds(0, 768)], wy_recv)
    for b in range(1, NX):
        piece = wall.at[pl.ds(pl.multiple_of(b * COLS + c * 128, 128), 128)]
        send(piece, piece, wc_send, wc_recv, (shuf_index(y, z, 1 - c), x))

    wait_for(got_y.at[pl.ds(0, NQ - 1)], line_recv.at[5])
    tile_stat[...] = pick(from_slot, got_y[...].reshape(SLOTS, 2 * COLS)).astype(BF16)
    for d in range(1, NX):
        rows = pl.ds(pl.multiple_of(lax.rem(x + d, NX) * 16, 16), 16)
        send(tile_stat.at[rows], peer_stat.at[NX - d - 1], st_send, st_recv, x_peer(d))
    for g in range(EARLY, GRPS):
        send_group(g)

    for a in aux[2:]:
        a.wait()
    wait_for(gb.at[pl.ds(0, NX - 1)], gb_recv)
    wait_for(wall.at[pl.ds(0, 3 * 128)], wc_recv)
    own_rows = pl.ds(pl.multiple_of(x * 16, 16), 16)
    stats = [tile_stat[own_rows, :]]
    wait_for(peer_stat, st_recv)
    stats += [peer_stat[d] for d in range(NX - 1)]
    for d in range(NX):
        s = stats[d].astype(F32)
        par[0, :, d * COLS:(d + 1) * COLS] = s[:, :COLS]
        par[1, :, d * COLS:(d + 1) * COLS] = s[:, COLS:] * gb[d, 0:1, :]

    @pl.loop(0, GRPS)
    def _(g):
        for d in range(1, NX):
            wait_for(raw.at[d - 1, pl.ds(0, GROWS)], x_recv.at[d - 1, g])
        for j in range(GROWS // TILE):
            t = g * (GROWS // TILE) + j
            for d in range(NX):
                cols = slice(d * COLS, (d + 1) * COLS)
                if d == 0:
                    first = x * OROWS + t * TILE
                    v = vals[pl.ds(pl.multiple_of(first, TILE), TILE), :]
                else:
                    v = raw[d - 1, pl.ds(pl.multiple_of(t * TILE, TILE), TILE), :]
                scored = (v.astype(F32) - par[0, pl.ds(t, 1), cols]) * par[1, pl.ds(t, 1), cols]
                lhs[j * TILE:(j + 1) * TILE, cols] = (scored + gb[d, 1:2, :]).astype(BF16)
        rows = pl.ds(pl.multiple_of(g * GROWS, GROWS), GROWS)
        out[rows, :] = jnp.dot(lhs[...], wall[...], preferred_element_type=F32).astype(BF16)

    wait_for(raw, x_send)
    wait_for(wall.at[pl.ds(0, 48), pl.ds(0, 256)], wx_send)
    wait_for(wall.at[pl.ds(0, (NX - 1) * (NZ - 1) * 16), pl.ds(0, 256)], wz_send)
    wait_for(wall.at[pl.ds(0, 3 * 128), pl.ds(0, 768)], wy_send)
    wait_for(wall.at[pl.ds(0, 3 * 128)], wc_send)
    wait_for(gb.at[pl.ds(0, NX - 1)], gb_send)
    wait_for(peer_stat, st_send)
    wait_for(tot_y.at[pl.ds(0, NQ - 1)], line_send.at[0])
    wait_for(buf_y.at[pl.ds(0, NQ - 1)], line_send.at[1])
    wait_for(tot_z.at[pl.ds(0, NZ - 1)], line_send.at[2])
    wait_for(buf_z.at[pl.ds(0, NZ - 1)], line_send.at[3])
    wait_for(got_z.at[pl.ds(0, NZ - 1)], line_send.at[4])
    wait_for(got_y.at[pl.ds(0, NQ - 1)], line_send.at[5])


def write_out(src, dst, sem):
    copies = []
    for i in range(4):
        rows = pl.ds(i * (OROWS // 4), OROWS // 4)
        copies.append(pltpu.make_async_copy(src.at[rows], dst.at[rows], sem.at[i]))
        copies[-1].start()
    for copy in copies:
        copy.wait()


def on_device(values, subgroup, owners, col_gain, col_bias, out_weight):
    dma, vmem = pltpu.SemaphoreType.DMA, pltpu.VMEM
    hbm = pl.BlockSpec(memory_space=pltpu.HBM)
    rows = pl.pallas_call(
        exchange,
        out_shape=pltpu.VMEM((OROWS, OUT), BF16),
        in_specs=[hbm] * 6,
        out_specs=pl.BlockSpec(memory_space=pltpu.VMEM),
        scratch_shapes=[
            vmem((ROWS, COLS), BF16),
            vmem((NX - 1, OROWS, COLS), BF16),
            vmem((NX * COLS, OUT), BF16),
            pltpu.SMEM((TILES,), jnp.int32),
            pltpu.SMEM((TILES,), jnp.int32),
            vmem((NX, 2, COLS), F32),
            vmem((TILES, 2 * COLS), F32),
            vmem((2, 1, 2 * COLS), F32),
            vmem((NQ, 1, 2 * COLS), F32),
            vmem((NZ, 1, 2 * COLS), F32),
            vmem((NQ, 16, MSG), BF16),
            vmem((NQ, 16, MSG), BF16),
            vmem((NZ, 16, MSG), BF16),
            vmem((NZ, 16, MSG), BF16),
            vmem((NZ, 16, 2 * COLS), BF16),
            vmem((NZ, 16, 2 * COLS), BF16),
            vmem((NQ, 16, 2 * COLS), BF16),
            vmem((NQ, 16, 2 * COLS), BF16),
            vmem((TILES, 2 * COLS), BF16),
            vmem((NX - 1, 16, 2 * COLS), BF16),
            vmem((2, 16, NX * COLS), F32),
            vmem((GROWS, NX * COLS), BF16),
            dma((8,)), dma((5,)), dma, dma((NX - 1, GRPS)),
            dma, dma, dma, dma, dma, dma, dma, dma, dma, dma, dma, dma,
            dma((6,)), dma((6,)),
            pltpu.SemaphoreType.REGULAR, pltpu.SemaphoreType.REGULAR,
        ],
        compiler_params=pltpu.CompilerParams(
            collective_id=0, has_side_effects=True, vmem_limit_bytes=32 * 1024 * 1024
        ),
    )(*(pltpu.with_memory_space_constraint(a, pltpu.HBM) for a in (values, subgroup, owners.reshape(TILES), col_gain, col_bias, out_weight)))
    return pl.pallas_call(
        write_out,
        out_shape=jax.ShapeDtypeStruct((OROWS, OUT), BF16),
        in_specs=[pl.BlockSpec(memory_space=pltpu.VMEM)],
        out_specs=pl.BlockSpec(memory_space=pltpu.HBM),
        scratch_shapes=[dma((4,))],
        compiler_params=pltpu.CompilerParams(vmem_limit_bytes=1024 * 1024),
    )(rows)


def solution(mesh):
    return jax.shard_map(
        on_device,
        mesh=mesh,
        in_specs=(P("shuf", "rep"), P("shuf"), P("shuf", None), P("rep"), P("rep"), P("rep", None)),
        out_specs=P(("shuf", "rep"), None),
        check_vma=False,
    )
```

```python
import jax
import jax.numpy as jnp
from jax import lax
from jax.experimental import pallas as pl
from jax.experimental.pallas import tpu as pltpu
from jax.sharding import PartitionSpec as P

TILE = 128
TILES = 64
GRP_DEV = 32
PRIOR = 256.0
COLS = 256
OUT = 1024
ROWS = 8192
OROWS = 2048
NX, NY, NZ, NC = 4, 4, 8, 2
NQ = NY * NC
SLOTS = 2 * NQ * NZ
GROWS = 256
PIECES = (512, 512, 512, 256, 128, 128)
STARTS = tuple(sum(PIECES[:k]) for k in range(len(PIECES)))
LAST = PIECES[-1]
KEPT = OROWS - LAST
EARLY = 3
HEAD = 1
ORDER = ((2, 2), (1, 1), (3, 3))
MSG = 2 * COLS + 128
MESH = pl.DeviceIdType.MESH
F32, BF16 = jnp.float32, jnp.bfloat16


def shuf_index(y, z, c):
    return (y * NZ + z) * NC + c


def iota(shape, dim):
    return lax.broadcasted_iota(jnp.int32, shape, dim)


def pick(matrix, rows):
    return jnp.dot(matrix, rows, preferred_element_type=F32)


def standardized(v, par, gb, t, d):
    cols = slice(d * COLS, (d + 1) * COLS)
    scored = (v.astype(F32) - par[0, pl.ds(t, 1), cols]) * par[1, pl.ds(t, 1), cols]
    return (scored + gb[d, 1:2, :]).astype(BF16)


def exchange(
    values, subgroup, owners, gain, bias, weight,
    out, last, own_last, wall, par, gb,
    vals, raw, subs, owns, tstat, totals, tot_y, tot_z,
    send_y, buf_y, send_z, buf_z, back_z, got_z, back_y, got_y, tile_stat, peer_stat, lhs,
    load_sem, aux_sem, x_send, x_recv, wx_send, wx_recv, wz_send, wz_recv, wy_send, wy_recv,
    wc_send, wc_recv, gb_send, gb_recv, st_send, st_recv, line_send, line_recv, near, lines, far,
):
    shuf, x = lax.axis_index("shuf"), lax.axis_index("rep")
    y, z, c = shuf // (NZ * NC), lax.rem(shuf // NC, NZ), lax.rem(shuf, NC)
    q = y * NC + c
    barrier = pltpu.get_barrier_semaphore()

    def x_peer(d):
        return (shuf, lax.rem(x + d, NX))

    def z_peer(d):
        return (shuf_index(y, lax.rem(z + d, NZ), c), x)

    def q_peer(d):
        p = lax.rem(q + d, NQ)
        return (shuf_index(p // NC, z, lax.rem(p, NC)), x)

    def signal(sem, to):
        pl.semaphore_signal(sem, inc=1, device_id=to, device_id_type=MESH)

    def send(src, dst, s, r, to):
        pltpu.make_async_remote_copy(src, dst, s, r, device_id=to, device_id_type=MESH).start()

    def wait_for(ref, sem):
        pltpu.make_async_copy(ref, ref, sem).wait()

    loads = []
    for i in range(8):
        part = pl.ds(i * 1024, 1024)
        loads.append(pltpu.make_async_copy(values.at[part], vals.at[part], load_sem.at[i]))
        loads[-1].start()
    aux = [
        pltpu.make_async_copy(subgroup, subs, aux_sem.at[0]),
        pltpu.make_async_copy(owners, owns, aux_sem.at[1]),
        pltpu.make_async_copy(weight, wall.at[pl.ds(0, COLS)], aux_sem.at[2]),
        pltpu.make_async_copy(gain, gb.at[0, 0], aux_sem.at[3]),
        pltpu.make_async_copy(bias, gb.at[0, 1], aux_sem.at[4]),
    ]
    for a in aux:
        a.start()

    is_head = x == HEAD

    @pl.when(is_head)
    def _():
        for d in range(1, NX):
            signal(barrier, x_peer(d))
        for d in range(1, NQ):
            signal(barrier, q_peer(d))
        for d in range(1, NZ):
            signal(barrier, z_peer(d))

    @pl.when(x != HEAD)
    def _():
        for d in range(1, NX):
            @pl.when(lax.rem(x + d, NX) != HEAD)
            def _():
                signal(barrier, x_peer(d))
        pl.semaphore_wait(barrier, NX - 1)
        signal(near, (shuf, HEAD))

    @pl.when(is_head)
    def _():
        pl.semaphore_wait(near, NX - 1)

    gathers = c == NC - 1
    w_cols = pl.ds(pl.multiple_of(y * 256, 256), 256)

    def w_rows(block):
        return pl.ds(pl.multiple_of(block * COLS + z * 32, 32), 32)

    for d in range(1, NX):
        at = NX - d
        send(gain, gb.at[at, 0], gb_send, gb_recv, x_peer(d))
        send(bias, gb.at[at, 1], gb_send, gb_recv, x_peer(d))

    @pl.when(gathers)
    def _():
        for d in range(1, NX):
            send(
                weight.at[w_rows(0), w_cols], wall.at[w_rows(NX - d), w_cols],
                wx_send, wx_recv, x_peer(d),
            )

    late_half = x // 2

    def send_piece(k):
        size = PIECES[k]
        for one, other in ORDER:
            d = one + (other - one) * late_half
            at = NX - 1 - d
            first = lax.rem(x + d, NX) * OROWS + STARTS[k]
            send(
                values.at[pl.ds(pl.multiple_of(first, LAST), size)],
                last.at[at] if k == len(PIECES) - 1 else raw.at[at, pl.ds(STARTS[k], size)],
                x_send.at[k // (len(PIECES) - 1)], x_recv.at[at, k], x_peer(d),
            )

    for k in range(EARLY):
        send_piece(k)

    @pl.when(is_head)
    def _():
        pl.semaphore_wait(barrier, NQ - 1 + NZ - 1)
        for d in range(1, NQ):
            signal(lines.at[0], q_peer(d))
        for d in range(1, NZ):
            signal(lines.at[1], z_peer(d))

    @pl.loop(0, 8)
    def _(i):
        wait_for(vals.at[pl.ds(0, 1024)], load_sem.at[i])

        @pl.loop(0, 8)
        def _(j):
            t = i * 8 + j
            a = jnp.zeros((8, COLS), F32)
            b = jnp.zeros((8, COLS), F32)
            for k in range(TILE // 16):
                v = vals[pl.ds(pl.multiple_of(t * TILE + k * 16, 16), 16), :].astype(F32)
                lo, hi = v[:8], v[8:]
                a = a + lo + hi
                b = b + lo * lo + hi * hi
            tstat[pl.ds(t, 1), :COLS] = jnp.sum(a, axis=0, keepdims=True)
            tstat[pl.ds(t, 1), COLS:] = jnp.sum(b, axis=0, keepdims=True)

    sums = tstat[...]
    own_total = jnp.sum(sums, axis=0, keepdims=True)
    totals[0] = own_total
    tot_y[q] = own_total

    for a in aux[:2]:
        a.wait()
    lane = iota((8, TILES), 1)
    own_row = jnp.zeros((8, TILES), jnp.int32)
    sub_row = jnp.zeros((8, TILES), jnp.int32)
    for t in range(TILES):
        own_row = jnp.where(lane == t, owns[t], own_row)
        sub_row = jnp.where(lane == t, subs[t], sub_row)
    i0, i1 = iota((TILES, TILES), 0), iota((TILES, TILES), 1)
    eye = i0 == i1

    def as_rows(row):
        return jnp.broadcast_to(row[:1], (TILES, TILES))

    def as_column(row):
        spread = jnp.where(eye, as_rows(row), 0).astype(F32)
        return jnp.sum(spread, axis=1, keepdims=True).astype(jnp.int32)

    same = (as_rows(own_row) == as_column(own_row)) & (i0 < i1)
    pos = jnp.sum(jnp.where(same, 1.0, 0.0), axis=0, keepdims=True).astype(jnp.int32)
    o = own_row[:1]
    slot = ((((o >> 4) * NC + (o & 1)) * NZ + ((o >> 1) & 7)) * 2) + pos
    slot_col = as_column(slot)
    to_slot = jnp.where(iota((SLOTS, TILES), 0) == slot, 1.0, 0.0).astype(BF16)
    from_slot = jnp.where(iota((TILES, SLOTS), 1) == slot_col, 1.0, 0.0).astype(BF16)
    label = jnp.where(iota((TILES, 128), 1) == as_column(sub_row), 1.0, 0.0).astype(BF16)
    packed = jnp.concatenate([sums.astype(BF16), label], axis=1)
    send_y[...] = pick(to_slot, packed).astype(BF16).reshape(NQ, 16, MSG)
    buf_y[q] = send_y[q]

    r0, r1 = iota((SLOTS, SLOTS), 0), iota((SLOTS, SLOTS), 1)
    swap = jnp.where(r1 == ((r0 >> 1) & 7) * 16 + (r0 >> 4) * 2 + (r0 & 1), 1.0, 0.0).astype(BF16)

    def line_known(i, peers):
        @pl.when(is_head)
        def _():
            pl.semaphore_wait(lines.at[i], peers)
            for d in range(1, NX):
                signal(far.at[i], x_peer(d))

        @pl.when(x != HEAD)
        def _():
            pl.semaphore_wait(far.at[i], 1)

    line_known(0, NQ - 1)
    for d in range(1, NQ):
        p = lax.rem(q + d, NQ)
        send(totals.at[0], tot_y.at[q], line_send.at[0], line_recv.at[0], q_peer(d))
        send(send_y.at[p], buf_y.at[q], line_send.at[1], line_recv.at[1], q_peer(d))

    line_known(1, NZ - 1)
    wx_all = wall.at[pl.ds(0, (NX - 1) * 32), pl.ds(0, 256)]
    wz_all = wall.at[pl.ds(0, (NX - 1) * (NZ - 1) * 32), pl.ds(0, 256)]
    wy_all = wall.at[pl.ds(0, (NX - 1) * COLS), pl.ds(0, 768)]
    foreign = wall.at[pl.ds(COLS, (NX - 1) * COLS)]

    @pl.when(gathers)
    def _():
        wait_for(wx_all, wx_recv)
        for d in range(1, NZ):
            for b in range(1, NX):
                piece = wall.at[w_rows(b), w_cols]
                send(piece, piece, wz_send, wz_recv, z_peer(d))

    wait_for(tot_y.at[pl.ds(0, NQ - 1)], line_recv.at[0])
    wait_for(buf_y.at[pl.ds(0, NQ - 1)], line_recv.at[1])
    line_total = jnp.sum(tot_y[...], axis=0)
    totals[1] = line_total
    tot_z[z] = line_total
    send_z[...] = pick(swap, buf_y[...].reshape(SLOTS, MSG)).astype(BF16).reshape(NZ, 16, MSG)
    buf_z[z] = send_z[z]
    for d in range(1, NZ):
        p = lax.rem(z + d, NZ)
        send(totals.at[1], tot_z.at[z], line_send.at[2], line_recv.at[2], z_peer(d))
        send(send_z.at[p], buf_z.at[z], line_send.at[3], line_recv.at[3], z_peer(d))

    @pl.when(gathers)
    def _():
        wait_for(wz_all, wz_recv)
        for d in range(1, NY):
            for b in range(1, NX):
                piece = wall.at[pl.ds(b * COLS, COLS), w_cols]
                send(piece, piece, wy_send, wy_recv, q_peer(NC * d))

    wait_for(tot_z.at[pl.ds(0, NZ - 1)], line_recv.at[2])
    wait_for(buf_z.at[pl.ds(0, NZ - 1)], line_recv.at[3])
    total = jnp.sum(tot_z[...], axis=0) / float(ROWS * NQ * NZ)
    arrived = buf_z[...].reshape(SLOTS, MSG)
    member = arrived[:, 2 * COLS:]
    member_t = jnp.transpose(member.astype(F32))[:GRP_DEV].astype(BF16)
    group = pick(member_t, arrived[:, : 2 * COLS])
    count = float(TILE) * jnp.sum(member_t.astype(F32), axis=1, keepdims=True)
    blended = (group + PRIOR * total) / (count + PRIOR)
    center, second = blended[:, :COLS], blended[:, COLS:]
    inverse = lax.rsqrt(second - center * center + 1e-05)
    both = jnp.concatenate([center, inverse], axis=1).astype(BF16)
    both = jnp.concatenate([both, jnp.zeros((128 - GRP_DEV, 2 * COLS), BF16)], axis=0)
    back_z[...] = pick(member, both).astype(BF16).reshape(NZ, 16, 2 * COLS)
    got_z[z] = back_z[z]
    for d in range(1, NZ):
        p = lax.rem(z + d, NZ)
        send(back_z.at[p], got_z.at[z], line_send.at[4], line_recv.at[4], z_peer(d))

    wait_for(got_z.at[pl.ds(0, NZ - 1)], line_recv.at[4])
    back_y[...] = pick(swap, got_z[...].reshape(SLOTS, 2 * COLS)).astype(BF16).reshape(NQ, 16, 2 * COLS)
    got_y[q] = back_y[q]
    for d in range(1, NQ):
        p = lax.rem(q + d, NQ)
        send(back_y.at[p], got_y.at[q], line_send.at[5], line_recv.at[5], q_peer(d))

    @pl.when(gathers)
    def _():
        wait_for(wy_all, wy_recv)
        send(foreign, foreign, wc_send, wc_recv, (shuf_index(y, z, 0), x))

    wait_for(got_y.at[pl.ds(0, NQ - 1)], line_recv.at[5])
    tile_stat[...] = pick(from_slot, got_y[...].reshape(SLOTS, 2 * COLS)).astype(BF16)
    for d in range(1, NX):
        rows = pl.ds(pl.multiple_of(lax.rem(x + d, NX) * 16, 16), 16)
        send(tile_stat.at[rows], peer_stat.at[NX - d - 1], st_send, st_recv, x_peer(d))
    for k in range(EARLY, len(PIECES)):
        send_piece(k)

    for a in aux[2:]:
        a.wait()
    wait_for(gb.at[pl.ds(0, NX - 1)], gb_recv)

    @pl.when(c == 0)
    def _():
        wait_for(foreign, wc_recv)

    own_rows = pl.ds(pl.multiple_of(x * 16, 16), 16)
    stats = [tile_stat[own_rows, :]]
    wait_for(peer_stat, st_recv)
    stats += [peer_stat[d] for d in range(NX - 1)]
    for d in range(NX):
        s = stats[d].astype(F32)
        par[0, :, d * COLS:(d + 1) * COLS] = s[:, :COLS]
        par[1, :, d * COLS:(d + 1) * COLS] = s[:, COLS:] * gb[d, 0:1, :]

    def own_scored(t):
        first = x * OROWS + t * TILE
        v = vals[pl.ds(pl.multiple_of(first, TILE), TILE), :]
        return standardized(v, par, gb, t, 0)

    def arrived_piece(k):
        for d in range(NX - 1):
            wait_for(last.at[d] if k == len(PIECES) - 1 else raw.at[d, pl.ds(0, PIECES[k])], x_recv.at[d, k])

    def project(first, count):
        for j in range(count // TILE):
            t = first // TILE + j
            at = slice(j * TILE, (j + 1) * TILE)
            lhs[at, :COLS] = own_scored(t)
            for d in range(1, NX):
                v = raw[d - 1, pl.ds(pl.multiple_of(t * TILE, TILE), TILE), :]
                lhs[at, d * COLS:(d + 1) * COLS] = standardized(v, par, gb, t, d)
        rows = pl.ds(pl.multiple_of(first, count), count)
        out[rows, :] = jnp.dot(lhs[:count, :], wall[...], preferred_element_type=F32).astype(BF16)

    for k in range(EARLY):
        arrived_piece(k)

    @pl.loop(0, STARTS[EARLY + 1] // GROWS)
    def _(g):
        @pl.when(g == STARTS[EARLY] // GROWS)
        def _():
            arrived_piece(EARLY)

        project(g * GROWS, GROWS)

    own_last[...] = own_scored(KEPT // TILE)
    arrived_piece(EARLY + 1)
    project(STARTS[EARLY + 1], PIECES[EARLY + 1])
    arrived_piece(EARLY + 2)

    wait_for(raw, x_send.at[0])
    wait_for(last, x_send.at[1])

    @pl.when(gathers)
    def _():
        wait_for(wx_all, wx_send)
        wait_for(wz_all, wz_send)
        wait_for(wy_all, wy_send)
        wait_for(foreign, wc_send)

    wait_for(gb.at[pl.ds(0, NX - 1)], gb_send)
    wait_for(peer_stat, st_send)
    wait_for(tot_y.at[pl.ds(0, NQ - 1)], line_send.at[0])
    wait_for(buf_y.at[pl.ds(0, NQ - 1)], line_send.at[1])
    wait_for(tot_z.at[pl.ds(0, NZ - 1)], line_send.at[2])
    wait_for(buf_z.at[pl.ds(0, NZ - 1)], line_send.at[3])
    wait_for(got_z.at[pl.ds(0, NZ - 1)], line_send.at[4])
    wait_for(got_y.at[pl.ds(0, NQ - 1)], line_send.at[5])


def finish(done, last, own_last, wall, par, gb, dst, lhs, rows, sem):
    early = pltpu.make_async_copy(done, dst.at[pl.ds(0, KEPT)], sem.at[0])
    early.start()
    lhs[:, :COLS] = own_last[...]
    for d in range(1, NX):
        lhs[:, d * COLS:(d + 1) * COLS] = standardized(last[d - 1], par, gb, KEPT // TILE, d)
    rows[...] = jnp.dot(lhs[...], wall[...], preferred_element_type=F32).astype(BF16)
    late = pltpu.make_async_copy(rows, dst.at[pl.ds(KEPT, LAST)], sem.at[1])
    late.start()
    early.wait()
    late.wait()


def on_device(values, subgroup, owners, col_gain, col_bias, out_weight):
    dma, vmem = pltpu.SemaphoreType.DMA, pltpu.VMEM
    hbm = pl.BlockSpec(memory_space=pltpu.HBM)
    results = [
        vmem((KEPT, OUT), BF16),
        vmem((NX - 1, LAST, COLS), BF16),
        vmem((LAST, COLS), BF16),
        vmem((NX * COLS, OUT), BF16),
        vmem((2, 16, NX * COLS), F32),
        vmem((NX, 2, COLS), F32),
    ]
    in_vmem = [pl.BlockSpec(memory_space=vmem)] * len(results)
    held = pl.pallas_call(
        exchange,
        out_shape=results,
        in_specs=[hbm] * 6,
        out_specs=in_vmem,
        scratch_shapes=[
            vmem((ROWS, COLS), BF16),
            vmem((NX - 1, KEPT, COLS), BF16),
            pltpu.SMEM((TILES,), jnp.int32),
            pltpu.SMEM((TILES,), jnp.int32),
            vmem((TILES, 2 * COLS), F32),
            vmem((2, 1, 2 * COLS), F32),
            vmem((NQ, 1, 2 * COLS), F32),
            vmem((NZ, 1, 2 * COLS), F32),
            vmem((NQ, 16, MSG), BF16),
            vmem((NQ, 16, MSG), BF16),
            vmem((NZ, 16, MSG), BF16),
            vmem((NZ, 16, MSG), BF16),
            vmem((NZ, 16, 2 * COLS), BF16),
            vmem((NZ, 16, 2 * COLS), BF16),
            vmem((NQ, 16, 2 * COLS), BF16),
            vmem((NQ, 16, 2 * COLS), BF16),
            vmem((TILES, 2 * COLS), BF16),
            vmem((NX - 1, 16, 2 * COLS), BF16),
            vmem((GROWS, NX * COLS), BF16),
            dma((8,)), dma((5,)), dma((2,)), dma((NX - 1, len(PIECES))),
            dma, dma, dma, dma, dma, dma, dma, dma, dma, dma, dma, dma,
            dma((6,)), dma((6,)),
            pltpu.SemaphoreType.REGULAR,
            pltpu.SemaphoreType.REGULAR((2,)), pltpu.SemaphoreType.REGULAR((2,)),
        ],
        compiler_params=pltpu.CompilerParams(
            collective_id=0, has_side_effects=True, vmem_limit_bytes=32 * 1024 * 1024
        ),
    )(*(
        pltpu.with_memory_space_constraint(a, pltpu.HBM)
        for a in (values, subgroup, owners.reshape(TILES), col_gain, col_bias, out_weight)
    ))
    return pl.pallas_call(
        finish,
        out_shape=jax.ShapeDtypeStruct((OROWS, OUT), BF16),
        in_specs=in_vmem,
        out_specs=hbm,
        scratch_shapes=[vmem((LAST, NX * COLS), BF16), vmem((LAST, OUT), BF16), dma((2,))],
        compiler_params=pltpu.CompilerParams(vmem_limit_bytes=8 * 1024 * 1024),
    )(*held)


def solution(mesh):
    return jax.shard_map(
        on_device,
        mesh=mesh,
        in_specs=(P("shuf", "rep"), P("shuf"), P("shuf", None), P("rep"), P("rep"), P("rep", None)),
        out_specs=P(("shuf", "rep"), None),
        check_vma=False,
    )
```

```python
import jax
import jax.numpy as jnp
from jax import lax
from jax.experimental import pallas as pl
from jax.experimental.pallas import tpu as pltpu
from jax.sharding import PartitionSpec as P

TILE = 128
TILES = 64
GRP_DEV = 32
PRIOR = 256.0
COLS = 256
OUT = 1024
ROWS = 8192
OROWS = 2048
NX, NY, NZ, NC = 4, 4, 8, 2
NQ = NY * NC
SLOTS = 2 * NQ * NZ
MSG = 2 * COLS + 128
GROWS = 256
PIECES = (512, 512, 512, 256, 128, 128)
STARTS = tuple(sum(PIECES[:k]) for k in range(len(PIECES)))
LAST = PIECES[-1]
KEPT = OROWS - LAST
SENT_BYTES = 2 * (
    (NX - 1) * (OROWS * COLS + 16 * 2 * COLS)
    + (NQ - 1 + NZ - 1) * 16 * (MSG + 2 * COLS)
)
W_BYTES = 2 * 256 * (NX - 1) * (32 + (NZ - 1) * 32 + (NY - 1) * COLS + 4 * COLS)
EARLY = 3
HEAD = 1
ORDER = ((2, 2), (1, 1), (3, 3))
MESH = pl.DeviceIdType.MESH
F32, BF16 = jnp.float32, jnp.bfloat16


def shuf_index(y, z, c):
    return (y * NZ + z) * NC + c


def iota(shape, dim):
    return lax.broadcasted_iota(jnp.int32, shape, dim)


def pick(matrix, rows):
    return jnp.dot(matrix, rows, preferred_element_type=F32)


def standardized(v, par, gb, t, d):
    cols = slice(d * COLS, (d + 1) * COLS)
    scored = (v.astype(F32) - par[0, pl.ds(t, 1), cols]) * par[1, pl.ds(t, 1), cols]
    return (scored + gb[d, 1:2, :]).astype(BF16)


def exchange(
    values, subgroup, owners, gain, bias, weight,
    out, last, own_last, wall, par, gb,
    vals, raw, subs, owns, tstat, totals, tots,
    send_y, buf_y, send_z, buf_z, back_z, got_z, back_y, got_y, tile_stat, peer_stat, lhs,
    load_sem, slot_sem, own_sem, sent, tot_sent, gb_sent, w_sent,
    x_recv, wx_recv, wz_recv, wy_recv, wc_recv, gb_recv, st_recv, line_recv, near, lines, far,
):
    shuf, x = lax.axis_index("shuf"), lax.axis_index("rep")
    y, z, c = shuf // (NZ * NC), lax.rem(shuf // NC, NZ), lax.rem(shuf, NC)
    q = y * NC + c
    barrier = pltpu.get_barrier_semaphore()
    tot_y, tot_z = tots.at[pl.ds(0, NQ)], tots.at[pl.ds(NQ, NZ)]

    def x_peer(d):
        return (shuf, lax.rem(x + d, NX))

    def z_peer(d):
        return (shuf_index(y, lax.rem(z + d, NZ), c), x)

    def q_peer(d):
        p = lax.rem(q + d, NQ)
        return (shuf_index(p // NC, z, lax.rem(p, NC)), x)

    def signal(sem, to):
        pl.semaphore_signal(sem, inc=1, device_id=to, device_id_type=MESH)

    def send(src, dst, s, r, to):
        pltpu.make_async_remote_copy(src, dst, s, r, device_id=to, device_id_type=MESH).start()

    def wait_for(ref, sem):
        pltpu.make_async_copy(ref, ref, sem).wait()

    pltpu.make_async_copy(values, vals, load_sem).start()
    aux = [
        pltpu.make_async_copy(subgroup, subs, slot_sem.at[0]),
        pltpu.make_async_copy(owners, owns, slot_sem.at[1]),
        pltpu.make_async_copy(weight, wall.at[pl.ds(0, COLS)], own_sem),
        pltpu.make_async_copy(gain, gb.at[0, 0], gb_recv),
        pltpu.make_async_copy(bias, gb.at[0, 1], gb_recv),
    ]
    for a in aux:
        a.start()

    is_head = x == HEAD

    @pl.when(is_head)
    def _():
        for d in range(1, NX):
            signal(barrier, x_peer(d))
        for d in range(1, NQ):
            signal(barrier, q_peer(d))
        for d in range(1, NZ):
            signal(barrier, z_peer(d))

    @pl.when(x != HEAD)
    def _():
        for d in range(1, NX):
            @pl.when(lax.rem(x + d, NX) != HEAD)
            def _():
                signal(barrier, x_peer(d))
        pl.semaphore_wait(barrier, NX - 1)
        signal(near, (shuf, HEAD))

    @pl.when(is_head)
    def _():
        pl.semaphore_wait(near, NX - 1)

    gathers = c == NC - 1
    w_cols = pl.ds(pl.multiple_of(y * 256, 256), 256)

    def w_rows(block):
        return pl.ds(pl.multiple_of(block * COLS + z * 32, 32), 32)

    for d in range(1, NX):
        at = NX - d
        send(gain, gb.at[at, 0], gb_sent, gb_recv, x_peer(d))
        send(bias, gb.at[at, 1], gb_sent, gb_recv, x_peer(d))

    @pl.when(gathers)
    def _():
        for d in range(1, NX):
            send(
                weight.at[w_rows(0), w_cols], wall.at[w_rows(NX - d), w_cols],
                w_sent, wx_recv, x_peer(d),
            )

    late_half = x // 2

    def send_piece(k):
        size = PIECES[k]
        for one, other in ORDER:
            d = one + (other - one) * late_half
            at = NX - 1 - d
            first = lax.rem(x + d, NX) * OROWS + STARTS[k]
            send(
                values.at[pl.ds(pl.multiple_of(first, LAST), size)],
                last.at[at] if k == len(PIECES) - 1 else raw.at[at, pl.ds(STARTS[k], size)],
                sent, x_recv.at[max(k - EARLY + 1, 0)], x_peer(d),
            )

    for k in range(EARLY):
        send_piece(k)

    @pl.when(is_head)
    def _():
        pl.semaphore_wait(barrier, NQ - 1 + NZ - 1)
        for d in range(1, NQ):
            signal(lines.at[0], q_peer(d))
        for d in range(1, NZ):
            signal(lines.at[1], z_peer(d))

    wait_for(vals, load_sem)

    @pl.loop(0, 8)
    def _(i):
        @pl.loop(0, 8)
        def _(j):
            t = i * 8 + j
            a = jnp.zeros((8, COLS), F32)
            b = jnp.zeros((8, COLS), F32)
            for k in range(TILE // 16):
                v = vals[pl.ds(pl.multiple_of(t * TILE + k * 16, 16), 16), :].astype(F32)
                lo, hi = v[:8], v[8:]
                a = a + lo + hi
                b = b + lo * lo + hi * hi
            tstat[pl.ds(t, 1), :COLS] = jnp.sum(a, axis=0, keepdims=True)
            tstat[pl.ds(t, 1), COLS:] = jnp.sum(b, axis=0, keepdims=True)

    sums = tstat[...]
    own_total = jnp.sum(sums, axis=0, keepdims=True)
    totals[0] = own_total
    tot_y[q] = own_total

    for a in aux[:2]:
        a.wait()
    lane = iota((8, TILES), 1)
    own_row = jnp.zeros((8, TILES), jnp.int32)
    sub_row = jnp.zeros((8, TILES), jnp.int32)
    for t in range(TILES):
        own_row = jnp.where(lane == t, owns[t], own_row)
        sub_row = jnp.where(lane == t, subs[t], sub_row)
    i0, i1 = iota((TILES, TILES), 0), iota((TILES, TILES), 1)
    eye = i0 == i1

    def as_rows(row):
        return jnp.broadcast_to(row[:1], (TILES, TILES))

    def as_column(row):
        spread = jnp.where(eye, as_rows(row), 0).astype(F32)
        return jnp.sum(spread, axis=1, keepdims=True).astype(jnp.int32)

    same = (as_rows(own_row) == as_column(own_row)) & (i0 < i1)
    pos = jnp.sum(jnp.where(same, 1.0, 0.0), axis=0, keepdims=True).astype(jnp.int32)
    o = own_row[:1]
    slot = ((((o >> 4) * NC + (o & 1)) * NZ + ((o >> 1) & 7)) * 2) + pos
    slot_col = as_column(slot)
    to_slot = jnp.where(iota((SLOTS, TILES), 0) == slot, 1.0, 0.0).astype(BF16)
    from_slot = jnp.where(iota((TILES, SLOTS), 1) == slot_col, 1.0, 0.0).astype(BF16)
    label = jnp.where(iota((TILES, 128), 1) == as_column(sub_row), 1.0, 0.0).astype(BF16)
    packed = jnp.concatenate([sums.astype(BF16), label], axis=1)
    send_y[...] = pick(to_slot, packed).astype(BF16).reshape(NQ, 16, MSG)
    buf_y[q] = send_y[q]

    r0, r1 = iota((SLOTS, SLOTS), 0), iota((SLOTS, SLOTS), 1)
    swap = jnp.where(r1 == ((r0 >> 1) & 7) * 16 + (r0 >> 4) * 2 + (r0 & 1), 1.0, 0.0).astype(BF16)

    def line_known(i, peers):
        @pl.when(is_head)
        def _():
            pl.semaphore_wait(lines.at[i], peers)
            for d in range(1, NX):
                signal(far.at[i], x_peer(d))

        @pl.when(x != HEAD)
        def _():
            pl.semaphore_wait(far.at[i], 1)

    line_known(0, NQ - 1)
    for d in range(1, NQ):
        p = lax.rem(q + d, NQ)
        send(totals.at[0], tot_y.at[q], tot_sent, line_recv.at[0], q_peer(d))
        send(send_y.at[p], buf_y.at[q], sent, line_recv.at[1], q_peer(d))

    line_known(1, NZ - 1)
    wx_all = wall.at[pl.ds(0, (NX - 1) * 32), pl.ds(0, 256)]
    wz_all = wall.at[pl.ds(0, (NX - 1) * (NZ - 1) * 32), pl.ds(0, 256)]
    wy_all = wall.at[pl.ds(0, (NX - 1) * COLS), pl.ds(0, 768)]
    foreign = wall.at[pl.ds(COLS, (NX - 1) * COLS)]

    @pl.when(gathers)
    def _():
        wait_for(wx_all, wx_recv)
        for d in range(1, NZ):
            for b in range(1, NX):
                piece = wall.at[w_rows(b), w_cols]
                send(piece, piece, w_sent, wz_recv, z_peer(d))

    wait_for(tot_y.at[pl.ds(0, NQ - 1)], line_recv.at[0])
    wait_for(buf_y.at[pl.ds(0, NQ - 1)], line_recv.at[1])
    line_total = jnp.sum(tot_y[...], axis=0)
    totals[1] = line_total
    tot_z[z] = line_total
    send_z[...] = pick(swap, buf_y[...].reshape(SLOTS, MSG)).astype(BF16).reshape(NZ, 16, MSG)
    buf_z[z] = send_z[z]
    for d in range(1, NZ):
        p = lax.rem(z + d, NZ)
        send(totals.at[1], tot_z.at[z], tot_sent, line_recv.at[2], z_peer(d))
        send(send_z.at[p], buf_z.at[z], sent, line_recv.at[3], z_peer(d))

    @pl.when(gathers)
    def _():
        wait_for(wz_all, wz_recv)
        for d in range(1, NY):
            for b in range(1, NX):
                piece = wall.at[pl.ds(b * COLS, COLS), w_cols]
                send(piece, piece, w_sent, wy_recv, q_peer(NC * d))

    wait_for(tot_z.at[pl.ds(0, NZ - 1)], line_recv.at[2])
    wait_for(buf_z.at[pl.ds(0, NZ - 1)], line_recv.at[3])
    total = jnp.sum(tot_z[...], axis=0) / float(ROWS * NQ * NZ)
    arrived = buf_z[...].reshape(SLOTS, MSG)
    member = arrived[:, 2 * COLS:]
    member_t = jnp.transpose(member.astype(F32))[:GRP_DEV].astype(BF16)
    group = pick(member_t, arrived[:, : 2 * COLS])
    count = float(TILE) * jnp.sum(member_t.astype(F32), axis=1, keepdims=True)
    blended = (group + PRIOR * total) / (count + PRIOR)
    center, second = blended[:, :COLS], blended[:, COLS:]
    inverse = lax.rsqrt(second - center * center + 1e-05)
    both = jnp.concatenate([center, inverse], axis=1).astype(BF16)
    both = jnp.concatenate([both, jnp.zeros((128 - GRP_DEV, 2 * COLS), BF16)], axis=0)
    back_z[...] = pick(member, both).astype(BF16).reshape(NZ, 16, 2 * COLS)
    got_z[z] = back_z[z]
    for d in range(1, NZ):
        p = lax.rem(z + d, NZ)
        send(back_z.at[p], got_z.at[z], sent, line_recv.at[4], z_peer(d))

    wait_for(got_z.at[pl.ds(0, NZ - 1)], line_recv.at[4])
    back_y[...] = pick(swap, got_z[...].reshape(SLOTS, 2 * COLS)).astype(BF16).reshape(NQ, 16, 2 * COLS)
    got_y[q] = back_y[q]
    for d in range(1, NQ):
        p = lax.rem(q + d, NQ)
        send(back_y.at[p], got_y.at[q], sent, line_recv.at[5], q_peer(d))

    @pl.when(gathers)
    def _():
        wait_for(wy_all, wy_recv)
        send(foreign, foreign, w_sent, wc_recv, (shuf_index(y, z, 0), x))

    wait_for(got_y.at[pl.ds(0, NQ - 1)], line_recv.at[5])
    tile_stat[...] = pick(from_slot, got_y[...].reshape(SLOTS, 2 * COLS)).astype(BF16)
    for d in range(1, NX):
        rows = pl.ds(pl.multiple_of(lax.rem(x + d, NX) * 16, 16), 16)
        send(tile_stat.at[rows], peer_stat.at[NX - d - 1], sent, st_recv, x_peer(d))
    for k in range(EARLY, len(PIECES)):
        send_piece(k)

    aux[2].wait()
    wait_for(gb, gb_recv)

    @pl.when(c == 0)
    def _():
        wait_for(foreign, wc_recv)

    own_rows = pl.ds(pl.multiple_of(x * 16, 16), 16)
    stats = [tile_stat[own_rows, :]]
    wait_for(peer_stat, st_recv)
    stats += [peer_stat[d] for d in range(NX - 1)]
    for d in range(NX):
        s = stats[d].astype(F32)
        par[0, :, d * COLS:(d + 1) * COLS] = s[:, :COLS]
        par[1, :, d * COLS:(d + 1) * COLS] = s[:, COLS:] * gb[d, 0:1, :]

    def own_scored(t):
        first = x * OROWS + t * TILE
        v = vals[pl.ds(pl.multiple_of(first, TILE), TILE), :]
        return standardized(v, par, gb, t, 0)

    def arrived_piece(k):
        rows = STARTS[EARLY] if k < EARLY else PIECES[k]
        whole = last if k == len(PIECES) - 1 else raw.at[:, pl.ds(0, rows)]
        wait_for(whole, x_recv.at[max(k - EARLY + 1, 0)])

    def project(first, count):
        for j in range(count // TILE):
            t = first // TILE + j
            at = slice(j * TILE, (j + 1) * TILE)
            lhs[at, :COLS] = own_scored(t)
            for d in range(1, NX):
                v = raw[d - 1, pl.ds(pl.multiple_of(t * TILE, TILE), TILE), :]
                lhs[at, d * COLS:(d + 1) * COLS] = standardized(v, par, gb, t, d)
        rows = pl.ds(pl.multiple_of(first, count), count)
        out[rows, :] = jnp.dot(lhs[:count, :], wall[...], preferred_element_type=F32).astype(BF16)

    arrived_piece(0)

    @pl.loop(0, STARTS[EARLY + 1] // GROWS)
    def _(g):
        @pl.when(g == STARTS[EARLY] // GROWS)
        def _():
            arrived_piece(EARLY)

        project(g * GROWS, GROWS)

    own_last[...] = own_scored(KEPT // TILE)
    arrived_piece(EARLY + 1)
    project(STARTS[EARLY + 1], PIECES[EARLY + 1])
    arrived_piece(EARLY + 2)

    wait_for(vals.at[pl.ds(0, SENT_BYTES // (2 * COLS))], sent)
    wait_for(tots.at[pl.ds(0, NQ + NZ - 2)], tot_sent)
    wait_for(gb.at[pl.ds(0, NX - 1)], gb_sent)

    @pl.when(gathers)
    def _():
        wait_for(vals.at[pl.ds(0, W_BYTES // (2 * COLS))], w_sent)


def finish(done, last, own_last, wall, par, gb, dst, lhs, rows, sem):
    early = pltpu.make_async_copy(done, dst.at[pl.ds(0, KEPT)], sem.at[0])
    early.start()
    lhs[:, :COLS] = own_last[...]
    for d in range(1, NX):
        lhs[:, d * COLS:(d + 1) * COLS] = standardized(last[d - 1], par, gb, KEPT // TILE, d)
    rows[...] = jnp.dot(lhs[...], wall[...], preferred_element_type=F32).astype(BF16)
    late = pltpu.make_async_copy(rows, dst.at[pl.ds(KEPT, LAST)], sem.at[1])
    late.start()
    early.wait()
    late.wait()


def on_device(values, subgroup, owners, col_gain, col_bias, out_weight):
    dma, vmem = pltpu.SemaphoreType.DMA, pltpu.VMEM
    hbm = pl.BlockSpec(memory_space=pltpu.HBM)
    results = [
        vmem((KEPT, OUT), BF16),
        vmem((NX - 1, LAST, COLS), BF16),
        vmem((LAST, COLS), BF16),
        vmem((NX * COLS, OUT), BF16),
        vmem((2, 16, NX * COLS), F32),
        vmem((NX, 2, COLS), F32),
    ]
    in_vmem = [pl.BlockSpec(memory_space=vmem)] * len(results)
    held = pl.pallas_call(
        exchange,
        out_shape=results,
        in_specs=[hbm] * 6,
        out_specs=in_vmem,
        scratch_shapes=[
            vmem((ROWS, COLS), BF16),
            vmem((NX - 1, KEPT, COLS), BF16),
            pltpu.SMEM((TILES,), jnp.int32),
            pltpu.SMEM((TILES,), jnp.int32),
            vmem((TILES, 2 * COLS), F32),
            vmem((2, 1, 2 * COLS), F32),
            vmem((NQ + NZ, 1, 2 * COLS), F32),
            vmem((NQ, 16, MSG), BF16),
            vmem((NQ, 16, MSG), BF16),
            vmem((NZ, 16, MSG), BF16),
            vmem((NZ, 16, MSG), BF16),
            vmem((NZ, 16, 2 * COLS), BF16),
            vmem((NZ, 16, 2 * COLS), BF16),
            vmem((NQ, 16, 2 * COLS), BF16),
            vmem((NQ, 16, 2 * COLS), BF16),
            vmem((TILES, 2 * COLS), BF16),
            vmem((NX - 1, 16, 2 * COLS), BF16),
            vmem((GROWS, NX * COLS), BF16),
            dma, dma((2,)), dma, dma, dma, dma, dma,
            dma((len(PIECES) - EARLY + 1,)), dma, dma, dma, dma, dma, dma, dma((6,)),
            pltpu.SemaphoreType.REGULAR,
            pltpu.SemaphoreType.REGULAR((2,)), pltpu.SemaphoreType.REGULAR((2,)),
        ],
        compiler_params=pltpu.CompilerParams(
            collective_id=0, has_side_effects=True, vmem_limit_bytes=32 * 1024 * 1024
        ),
    )(*(
        pltpu.with_memory_space_constraint(a, pltpu.HBM)
        for a in (values, subgroup, owners.reshape(TILES), col_gain, col_bias, out_weight)
    ))
    return pl.pallas_call(
        finish,
        out_shape=jax.ShapeDtypeStruct((OROWS, OUT), BF16),
        in_specs=in_vmem,
        out_specs=hbm,
        scratch_shapes=[vmem((LAST, NX * COLS), BF16), vmem((LAST, OUT), BF16), dma((2,))],
        compiler_params=pltpu.CompilerParams(vmem_limit_bytes=8 * 1024 * 1024),
    )(*held)


def solution(mesh):
    return jax.shard_map(
        on_device,
        mesh=mesh,
        in_specs=(P("shuf", "rep"), P("shuf"), P("shuf", None), P("rep"), P("rep"), P("rep", None)),
        out_specs=P(("shuf", "rep"), None),
        check_vma=False,
    )
```

```python
import jax
import jax.numpy as jnp
from jax import lax
from jax.experimental import pallas as pl
from jax.experimental.pallas import tpu as pltpu
from jax.sharding import PartitionSpec as P

TILE = 128
TILES = 64
GRP_DEV = 32
PRIOR = 256.0
COLS = 256
OUT = 1024
ROWS = 8192
OROWS = 2048
NX, NY, NZ, NC = 4, 4, 8, 2
NQ = NY * NC
SLOTS = 2 * NQ * NZ
MSG = 2 * COLS + 128
GROWS = 256
PIECES = (512, 512, 512, 256, 128, 128)
STARTS = tuple(sum(PIECES[:k]) for k in range(len(PIECES)))
LAST = PIECES[-1]
KEPT = OROWS - LAST
SENT_BYTES = 2 * (
    (NX - 1) * (OROWS * COLS + 16 * 2 * COLS)
    + (NQ - 1 + NZ - 1) * 16 * (MSG + 2 * COLS)
)
W_BYTES = 2 * 256 * (NX - 1) * (32 + (NZ - 1) * 32 + (NY - 1) * COLS + 4 * COLS)
EARLY = 3
HEAD = 1
ORDER = ((2, 2), (1, 1), (3, 3))
MESH = pl.DeviceIdType.MESH
F32, BF16 = jnp.float32, jnp.bfloat16


def shuf_index(y, z, c):
    return (y * NZ + z) * NC + c


def iota(shape, dim):
    return lax.broadcasted_iota(jnp.int32, shape, dim)


def pick(matrix, rows):
    return jnp.dot(matrix, rows, preferred_element_type=F32)


def standardized(v, par, gb, t, d):
    cols = slice(d * COLS, (d + 1) * COLS)
    scored = (v.astype(F32) - par[0, pl.ds(t, 1), cols]) * par[1, pl.ds(t, 1), cols]
    return (scored + gb[d, 1:2, :]).astype(BF16)


def exchange(
    values, subgroup, owners, gain, bias, weight,
    out, last, own_last, wall, par, gb,
    vals, raw, subs, owns, tstat, totals, tots,
    send_y, buf_y, send_z, buf_z, back_z, got_z, back_y, got_y, tile_stat, peer_stat, lhs,
    load_sem, slot_sem, own_sem, sent, tot_sent, w_sent,
    x_recv, wx_recv, wz_recv, wy_recv, wc_recv, gb_recv, st_recv, line_recv, near, lines, far,
):
    shuf, x = lax.axis_index("shuf"), lax.axis_index("rep")
    y, z, c = shuf // (NZ * NC), lax.rem(shuf // NC, NZ), lax.rem(shuf, NC)
    q = y * NC + c
    barrier = pltpu.get_barrier_semaphore()
    tot_y, tot_z = tots.at[pl.ds(0, NQ)], tots.at[pl.ds(NQ, NZ)]

    def x_peer(d):
        return (shuf, lax.rem(x + d, NX))

    def z_peer(d):
        return (shuf_index(y, lax.rem(z + d, NZ), c), x)

    def q_peer(d):
        p = lax.rem(q + d, NQ)
        return (shuf_index(p // NC, z, lax.rem(p, NC)), x)

    def signal(sem, to):
        pl.semaphore_signal(sem, inc=1, device_id=to, device_id_type=MESH)

    def send(src, dst, s, r, to):
        pltpu.make_async_remote_copy(src, dst, s, r, device_id=to, device_id_type=MESH).start()

    def wait_for(ref, sem):
        pltpu.make_async_copy(ref, ref, sem).wait()

    pltpu.make_async_copy(values, vals, load_sem).start()
    aux = [
        pltpu.make_async_copy(subgroup, subs, slot_sem.at[0]),
        pltpu.make_async_copy(owners, owns, slot_sem.at[1]),
        pltpu.make_async_copy(weight, wall.at[pl.ds(0, COLS)], own_sem),
        pltpu.make_async_copy(gain, gb.at[0, 0], gb_recv),
        pltpu.make_async_copy(bias, gb.at[0, 1], gb_recv),
    ]
    for a in aux:
        a.start()

    is_head = x == HEAD

    @pl.when(is_head)
    def _():
        for d in range(1, NX):
            signal(barrier, x_peer(d))
        for d in range(1, NQ):
            signal(barrier, q_peer(d))
        for d in range(1, NZ):
            signal(barrier, z_peer(d))

    @pl.when(x != HEAD)
    def _():
        for d in range(1, NX):
            @pl.when(lax.rem(x + d, NX) != HEAD)
            def _():
                signal(barrier, x_peer(d))
        pl.semaphore_wait(barrier, NX - 1)
        signal(near, (shuf, HEAD))

    @pl.when(is_head)
    def _():
        pl.semaphore_wait(near, NX - 1)

    gathers = c == NC - 1
    w_cols = pl.ds(pl.multiple_of(y * 256, 256), 256)

    def w_rows(block):
        return pl.ds(pl.multiple_of(block * COLS + z * 32, 32), 32)

    for d in range(1, NX):
        at = NX - d
        send(gain, gb.at[at, 0], tot_sent, gb_recv, x_peer(d))
        send(bias, gb.at[at, 1], tot_sent, gb_recv, x_peer(d))

    @pl.when(gathers)
    def _():
        for d in range(1, NX):
            send(
                weight.at[w_rows(0), w_cols], wall.at[w_rows(NX - d), w_cols],
                w_sent, wx_recv, x_peer(d),
            )

    late_half = x // 2

    def send_piece(k):
        size = PIECES[k]
        for one, other in ORDER:
            d = one + (other - one) * late_half
            at = NX - 1 - d
            first = lax.rem(x + d, NX) * OROWS + STARTS[k]
            send(
                values.at[pl.ds(pl.multiple_of(first, LAST), size)],
                last.at[at] if k == len(PIECES) - 1 else raw.at[at, pl.ds(STARTS[k], size)],
                sent, x_recv.at[max(k - EARLY + 1, 0)], x_peer(d),
            )

    for k in range(EARLY):
        send_piece(k)

    @pl.when(is_head)
    def _():
        pl.semaphore_wait(barrier, NQ - 1 + NZ - 1)
        for d in range(1, NQ):
            signal(lines, q_peer(d))
        for d in range(1, NZ):
            signal(lines, z_peer(d))

    wait_for(vals, load_sem)

    @pl.loop(0, 8)
    def _(i):
        @pl.loop(0, 8)
        def _(j):
            t = i * 8 + j
            a = jnp.zeros((8, COLS), F32)
            b = jnp.zeros((8, COLS), F32)
            for k in range(TILE // 16):
                v = vals[pl.ds(pl.multiple_of(t * TILE + k * 16, 16), 16), :].astype(F32)
                lo, hi = v[:8], v[8:]
                a = a + lo + hi
                b = b + lo * lo + hi * hi
            tstat[pl.ds(t, 1), :COLS] = jnp.sum(a, axis=0, keepdims=True)
            tstat[pl.ds(t, 1), COLS:] = jnp.sum(b, axis=0, keepdims=True)

    sums = tstat[...]
    own_total = jnp.sum(sums, axis=0, keepdims=True)
    totals[0] = own_total
    tot_y[q] = own_total

    for a in aux[:2]:
        a.wait()
    lane = iota((8, TILES), 1)
    own_row = jnp.zeros((8, TILES), jnp.int32)
    sub_row = jnp.zeros((8, TILES), jnp.int32)
    for t in range(TILES):
        own_row = jnp.where(lane == t, owns[t], own_row)
        sub_row = jnp.where(lane == t, subs[t], sub_row)
    i0, i1 = iota((TILES, TILES), 0), iota((TILES, TILES), 1)
    eye = i0 == i1

    def as_rows(row):
        return jnp.broadcast_to(row[:1], (TILES, TILES))

    def as_column(row):
        spread = jnp.where(eye, as_rows(row), 0).astype(F32)
        return jnp.sum(spread, axis=1, keepdims=True).astype(jnp.int32)

    same = (as_rows(own_row) == as_column(own_row)) & (i0 < i1)
    pos = jnp.sum(jnp.where(same, 1.0, 0.0), axis=0, keepdims=True).astype(jnp.int32)
    o = own_row[:1]
    slot = ((((o >> 4) * NC + (o & 1)) * NZ + ((o >> 1) & 7)) * 2) + pos
    slot_col = as_column(slot)
    to_slot = jnp.where(iota((SLOTS, TILES), 0) == slot, 1.0, 0.0).astype(BF16)
    from_slot = jnp.where(iota((TILES, SLOTS), 1) == slot_col, 1.0, 0.0).astype(BF16)
    label = jnp.where(iota((TILES, 128), 1) == as_column(sub_row), 1.0, 0.0).astype(BF16)
    packed = jnp.concatenate([sums.astype(BF16), label], axis=1)
    send_y[...] = pick(to_slot, packed).astype(BF16).reshape(NQ, 16, MSG)
    buf_y[q] = send_y[q]

    r0, r1 = iota((SLOTS, SLOTS), 0), iota((SLOTS, SLOTS), 1)
    swap = jnp.where(r1 == ((r0 >> 1) & 7) * 16 + (r0 >> 4) * 2 + (r0 & 1), 1.0, 0.0).astype(BF16)

    @pl.when(is_head)
    def _():
        pl.semaphore_wait(lines, NQ - 1 + NZ - 1)
        for d in range(1, NX):
            signal(far, x_peer(d))

    @pl.when(x != HEAD)
    def _():
        pl.semaphore_wait(far, 1)

    for d in range(1, NQ):
        p = lax.rem(q + d, NQ)
        send(totals.at[0], tot_y.at[q], tot_sent, line_recv.at[0], q_peer(d))
        send(send_y.at[p], buf_y.at[q], sent, line_recv.at[1], q_peer(d))

    wx_all = wall.at[pl.ds(0, (NX - 1) * 32), pl.ds(0, 256)]
    wz_all = wall.at[pl.ds(0, (NX - 1) * (NZ - 1) * 32), pl.ds(0, 256)]
    wy_all = wall.at[pl.ds(0, (NX - 1) * COLS), pl.ds(0, 768)]
    foreign = wall.at[pl.ds(COLS, (NX - 1) * COLS)]

    @pl.when(gathers)
    def _():
        wait_for(wx_all, wx_recv)
        for d in range(1, NZ):
            for b in range(1, NX):
                piece = wall.at[w_rows(b), w_cols]
                send(piece, piece, w_sent, wz_recv, z_peer(d))

    wait_for(tot_y.at[pl.ds(0, NQ - 1)], line_recv.at[0])
    wait_for(buf_y.at[pl.ds(0, NQ - 1)], line_recv.at[1])
    line_total = jnp.sum(tot_y[...], axis=0)
    totals[1] = line_total
    tot_z[z] = line_total
    send_z[...] = pick(swap, buf_y[...].reshape(SLOTS, MSG)).astype(BF16).reshape(NZ, 16, MSG)
    buf_z[z] = send_z[z]
    for d in range(1, NZ):
        p = lax.rem(z + d, NZ)
        send(totals.at[1], tot_z.at[z], tot_sent, line_recv.at[2], z_peer(d))
        send(send_z.at[p], buf_z.at[z], sent, line_recv.at[3], z_peer(d))

    @pl.when(gathers)
    def _():
        wait_for(wz_all, wz_recv)
        for d in range(1, NY):
            for b in range(1, NX):
                piece = wall.at[pl.ds(b * COLS, COLS), w_cols]
                send(piece, piece, w_sent, wy_recv, q_peer(NC * d))

    wait_for(tot_z.at[pl.ds(0, NZ - 1)], line_recv.at[2])
    wait_for(buf_z.at[pl.ds(0, NZ - 1)], line_recv.at[3])
    total = jnp.sum(tot_z[...], axis=0) / float(ROWS * NQ * NZ)
    arrived = buf_z[...].reshape(SLOTS, MSG)
    member = arrived[:, 2 * COLS:]
    member_t = jnp.transpose(member.astype(F32))[:GRP_DEV].astype(BF16)
    group = pick(member_t, arrived[:, : 2 * COLS])
    count = float(TILE) * jnp.sum(member_t.astype(F32), axis=1, keepdims=True)
    blended = (group + PRIOR * total) / (count + PRIOR)
    center, second = blended[:, :COLS], blended[:, COLS:]
    inverse = lax.rsqrt(second - center * center + 1e-05)
    both = jnp.concatenate([center, inverse], axis=1).astype(BF16)
    both = jnp.concatenate([both, jnp.zeros((128 - GRP_DEV, 2 * COLS), BF16)], axis=0)
    back_z[...] = pick(member, both).astype(BF16).reshape(NZ, 16, 2 * COLS)
    got_z[z] = back_z[z]
    for d in range(1, NZ):
        p = lax.rem(z + d, NZ)
        send(back_z.at[p], got_z.at[z], sent, line_recv.at[4], z_peer(d))

    wait_for(got_z.at[pl.ds(0, NZ - 1)], line_recv.at[4])
    back_y[...] = pick(swap, got_z[...].reshape(SLOTS, 2 * COLS)).astype(BF16).reshape(NQ, 16, 2 * COLS)
    got_y[q] = back_y[q]
    for d in range(1, NQ):
        p = lax.rem(q + d, NQ)
        send(back_y.at[p], got_y.at[q], sent, line_recv.at[5], q_peer(d))

    @pl.when(gathers)
    def _():
        wait_for(wy_all, wy_recv)
        send(foreign, foreign, w_sent, wc_recv, (shuf_index(y, z, 0), x))

    wait_for(got_y.at[pl.ds(0, NQ - 1)], line_recv.at[5])
    tile_stat[...] = pick(from_slot, got_y[...].reshape(SLOTS, 2 * COLS)).astype(BF16)
    for d in range(1, NX):
        rows = pl.ds(pl.multiple_of(lax.rem(x + d, NX) * 16, 16), 16)
        send(tile_stat.at[rows], peer_stat.at[NX - d - 1], sent, st_recv, x_peer(d))
    for k in range(EARLY, len(PIECES)):
        send_piece(k)

    aux[2].wait()
    wait_for(gb, gb_recv)

    @pl.when(c == 0)
    def _():
        wait_for(foreign, wc_recv)

    own_rows = pl.ds(pl.multiple_of(x * 16, 16), 16)
    stats = [tile_stat[own_rows, :]]
    wait_for(peer_stat, st_recv)
    stats += [peer_stat[d] for d in range(NX - 1)]
    for d in range(NX):
        s = stats[d].astype(F32)
        par[0, :, d * COLS:(d + 1) * COLS] = s[:, :COLS]
        par[1, :, d * COLS:(d + 1) * COLS] = s[:, COLS:] * gb[d, 0:1, :]

    def own_scored(t):
        first = x * OROWS + t * TILE
        v = vals[pl.ds(pl.multiple_of(first, TILE), TILE), :]
        return standardized(v, par, gb, t, 0)

    def arrived_piece(k):
        rows = STARTS[EARLY] if k < EARLY else PIECES[k]
        whole = last if k == len(PIECES) - 1 else raw.at[:, pl.ds(0, rows)]
        wait_for(whole, x_recv.at[max(k - EARLY + 1, 0)])

    def project(first, count):
        for j in range(count // TILE):
            t = first // TILE + j
            at = slice(j * TILE, (j + 1) * TILE)
            lhs[at, :COLS] = own_scored(t)
            for d in range(1, NX):
                v = raw[d - 1, pl.ds(pl.multiple_of(t * TILE, TILE), TILE), :]
                lhs[at, d * COLS:(d + 1) * COLS] = standardized(v, par, gb, t, d)
        rows = pl.ds(pl.multiple_of(first, count), count)
        out[rows, :] = jnp.dot(lhs[:count, :], wall[...], preferred_element_type=F32).astype(BF16)

    arrived_piece(0)

    @pl.loop(0, STARTS[EARLY + 1] // GROWS)
    def _(g):
        @pl.when(g == STARTS[EARLY] // GROWS)
        def _():
            arrived_piece(EARLY)

        project(g * GROWS, GROWS)

    own_last[...] = own_scored(KEPT // TILE)
    arrived_piece(EARLY + 1)
    project(STARTS[EARLY + 1], PIECES[EARLY + 1])
    arrived_piece(EARLY + 2)

    wait_for(vals.at[pl.ds(0, SENT_BYTES // (2 * COLS))], sent)
    wait_for(tots.at[pl.ds(0, NQ + NZ - 2 + NX - 1)], tot_sent)

    @pl.when(gathers)
    def _():
        wait_for(vals.at[pl.ds(0, W_BYTES // (2 * COLS))], w_sent)


def finish(done, last, own_last, wall, par, gb, dst, lhs, rows, sem):
    early = pltpu.make_async_copy(done, dst.at[pl.ds(0, KEPT)], sem.at[0])
    early.start()
    lhs[:, :COLS] = own_last[...]
    for d in range(1, NX):
        lhs[:, d * COLS:(d + 1) * COLS] = standardized(last[d - 1], par, gb, KEPT // TILE, d)
    rows[...] = jnp.dot(lhs[...], wall[...], preferred_element_type=F32).astype(BF16)
    late = pltpu.make_async_copy(rows, dst.at[pl.ds(KEPT, LAST)], sem.at[1])
    late.start()
    early.wait()
    late.wait()


def on_device(values, subgroup, owners, col_gain, col_bias, out_weight):
    dma, vmem = pltpu.SemaphoreType.DMA, pltpu.VMEM
    hbm = pl.BlockSpec(memory_space=pltpu.HBM)
    results = [
        vmem((KEPT, OUT), BF16),
        vmem((NX - 1, LAST, COLS), BF16),
        vmem((LAST, COLS), BF16),
        vmem((NX * COLS, OUT), BF16),
        vmem((2, 16, NX * COLS), F32),
        vmem((NX, 2, COLS), F32),
    ]
    in_vmem = [pl.BlockSpec(memory_space=vmem)] * len(results)
    held = pl.pallas_call(
        exchange,
        out_shape=results,
        in_specs=[hbm] * 6,
        out_specs=in_vmem,
        scratch_shapes=[
            vmem((ROWS, COLS), BF16),
            vmem((NX - 1, KEPT, COLS), BF16),
            pltpu.SMEM((TILES,), jnp.int32),
            pltpu.SMEM((TILES,), jnp.int32),
            vmem((TILES, 2 * COLS), F32),
            vmem((2, 1, 2 * COLS), F32),
            vmem((NQ + NZ + 1, 1, 2 * COLS), F32),
            vmem((NQ, 16, MSG), BF16),
            vmem((NQ, 16, MSG), BF16),
            vmem((NZ, 16, MSG), BF16),
            vmem((NZ, 16, MSG), BF16),
            vmem((NZ, 16, 2 * COLS), BF16),
            vmem((NZ, 16, 2 * COLS), BF16),
            vmem((NQ, 16, 2 * COLS), BF16),
            vmem((NQ, 16, 2 * COLS), BF16),
            vmem((TILES, 2 * COLS), BF16),
            vmem((NX - 1, 16, 2 * COLS), BF16),
            vmem((GROWS, NX * COLS), BF16),
            dma, dma((2,)), dma, dma, dma, dma,
            dma((len(PIECES) - EARLY + 1,)), dma, dma, dma, dma, dma, dma, dma((6,)),
            pltpu.SemaphoreType.REGULAR,
            pltpu.SemaphoreType.REGULAR, pltpu.SemaphoreType.REGULAR,
        ],
        compiler_params=pltpu.CompilerParams(
            collective_id=0, has_side_effects=True, vmem_limit_bytes=32 * 1024 * 1024
        ),
    )(*(
        pltpu.with_memory_space_constraint(a, pltpu.HBM)
        for a in (values, subgroup, owners.reshape(TILES), col_gain, col_bias, out_weight)
    ))
    return pl.pallas_call(
        finish,
        out_shape=jax.ShapeDtypeStruct((OROWS, OUT), BF16),
        in_specs=in_vmem,
        out_specs=hbm,
        scratch_shapes=[vmem((LAST, NX * COLS), BF16), vmem((LAST, OUT), BF16), dma((2,))],
        compiler_params=pltpu.CompilerParams(vmem_limit_bytes=8 * 1024 * 1024),
    )(*held)


def solution(mesh):
    return jax.shard_map(
        on_device,
        mesh=mesh,
        in_specs=(P("shuf", "rep"), P("shuf"), P("shuf", None), P("rep"), P("rep"), P("rep", None)),
        out_specs=P(("shuf", "rep"), None),
        check_vma=False,
    )
```
